16 devices in a mesh: dp: 4 (over y, z, core), tp: 4 (over x).
Axes of the slice: x: 4, y: 2, z: 1, core: 2. Of those that a mesh axis runs over, the one named last changes fastest.
The devices are a block of a 4x4x8 slice.
Arguments:
- x: bfloat16 [8192, 2560], P(('dp', 'tp')), parts along dimension 0
- gain_a: bfloat16 [2560], replicated
- wq: bfloat16 [2560, 4096], P(None, 'tp')
- wk: bfloat16 [2560, 1024], P(None, 'tp')
- wv: bfloat16 [2560, 1024], P(None, 'tp')
- wo: bfloat16 [4096, 2560], P('tp')
- gain_m: bfloat16 [2560], replicated
- w_gate: bfloat16 [2560, 9728], P(None, 'tp')
- w_up: bfloat16 [2560, 9728], P(None, 'tp')
- w_down: bfloat16 [9728, 2560], P('tp')
Outputs:
- output: bfloat16 [8192, 2560], P(('dp', 'tp')), parts along dimension 0
There are 4 independent parts. The reference program is written for one: setup_inputs(seed, part) draws one part's arguments, and reference() takes and returns one part's arrays. A program takes and returns all parts, laid end to end along the dimension named above; an argument that names none is the same for every part.
All inputs are finite; a program needn't handle non-finite values.
Results may differ from the reference program's by a relative error of at most 0.017.
Values are sent between devices in bfloat16 or wider.
A program may use at most 768 MiB of HBM per device.

```python
import jax
import jax.numpy as jnp
from jax import lax

ROWS = 2048
D = 2560
HEADS = 32
KV_HEADS = 8
HEAD = 128
FF = 9728
THETA = 10000


def setup_inputs(seed: int = 0, part: int = 0) -> dict:
    kx, kn, kq, kk, kv, ko, km, kg, ku, kd = jax.random.split(jax.random.key(seed), 10)

    def weights(key, rows, columns):
        return jax.random.normal(key, (rows, columns), jnp.float32) * rows**-0.5

    drawn = {
        "x": jax.random.normal(jax.random.fold_in(kx, part), (ROWS, D), jnp.float32),
        "gain_a": 1 + 0.1 * jax.random.normal(kn, (D,), jnp.float32),
        "wq": 2 * weights(kq, D, HEADS * HEAD),
        "wk": 2 * weights(kk, D, KV_HEADS * HEAD),
        "wv": 4 * weights(kv, D, KV_HEADS * HEAD),
        "wo": weights(ko, HEADS * HEAD, D),
        "gain_m": 1 + 0.1 * jax.random.normal(km, (D,), jnp.float32),
        "w_gate": weights(kg, D, FF),
        "w_up": weights(ku, D, FF),
        "w_down": 2 * weights(kd, FF, D),
    }
    return {k: v.astype(jnp.bfloat16) for k, v in drawn.items()}


def normed(x, gain):
    wide = x.astype(jnp.float32)
    scale = lax.rsqrt(jnp.mean(wide * wide, -1, keepdims=True) + 1e-6)
    return (wide * scale * gain.astype(jnp.float32)).astype(jnp.bfloat16)


def turned(t, place, theta):
    half = t.shape[-1] // 2
    angle = place.astype(jnp.float32)[:, None] * theta ** (-jnp.arange(half, dtype=jnp.float32) / half)
    cos, sin = jnp.cos(angle)[:, None], jnp.sin(angle)[:, None]
    a, b = t[..., :half].astype(jnp.float32), t[..., half:].astype(jnp.float32)
    return jnp.concatenate([a * cos - b * sin, b * cos + a * sin], -1).astype(jnp.bfloat16)


def matmul(a, w):
    return jnp.dot(a, w, preferred_element_type=jnp.float32).astype(jnp.bfloat16)


def einsum(form, a, b):
    return jnp.einsum(form, a.astype(jnp.float32), b.astype(jnp.float32))


def attention(q, k, v):
    scores = einsum("tgsd,ugd->gstu", q, k) * q.shape[-1] ** -0.5
    token = jnp.arange(q.shape[0])
    scores = jnp.where(token[:, None] >= token, scores, -jnp.inf)
    weights = jax.nn.softmax(scores, -1).astype(jnp.bfloat16)
    return einsum("gstu,ugd->tgsd", weights, v).astype(jnp.bfloat16)


def reference(x, gain_a, wq, wk, wv, wo, gain_m, w_gate, w_up, w_down):
    a, place = normed(x, gain_a), jnp.arange(ROWS)
    q = turned(matmul(a, wq).reshape(ROWS, HEADS, HEAD), place, THETA).reshape(ROWS, KV_HEADS, -1, HEAD)
    k = turned(matmul(a, wk).reshape(ROWS, KV_HEADS, HEAD), place, THETA)
    v = matmul(a, wv).reshape(ROWS, KV_HEADS, HEAD)
    seen = attention(q, k, v).reshape(ROWS, HEADS * HEAD)
    h = (x.astype(jnp.float32) + jnp.dot(seen, wo, preferred_element_type=jnp.float32)).astype(jnp.bfloat16)
    b = normed(h, gain_m)
    gate = jnp.dot(b, w_gate, preferred_element_type=jnp.float32)
    up = jnp.dot(b, w_up, preferred_element_type=jnp.float32)
    hidden = (jax.nn.silu(gate) * up).astype(jnp.bfloat16)
    return (h.astype(jnp.float32) + jnp.dot(hidden, w_down, preferred_element_type=jnp.float32)).astype(jnp.bfloat16)
```

```python
import jax
import jax.numpy as jnp
from jax import lax
from jax.experimental import pallas as pl
from jax.experimental.pallas import tpu as pltpu

NEG = -1e30
HIDDEN = 2 * NEG
LOG2E = 1.4426950408889634


def _dot(a, b, ca, cb):
    return lax.dot_general(a, b, (((ca,), (cb,)), ((), ())), preferred_element_type=jnp.float32)


from jax.sharding import PartitionSpec as P

HEAD = 128
THETA = 10000
OWN, RIGHT, FAR, LEFT = 0, 1, 2, 3
PARTS = 4
MOST = 67_043_328
KINDS = 5


class Ring:
    def __init__(self, blocks, halves, sums, send, recv):
        self.blocks, self.halves, self.sums, self.send, self.recv = blocks, halves, sums, send, recv
        n = lax.axis_size("tp")
        self.me = lax.axis_index("tp")
        self.to = (lax.rem(self.me + 1, n), lax.rem(self.me + n - 1, n))
        rows = blocks.shape[2]
        self.top, self.low = pl.ds(0, rows // 2), pl.ds(rows // 2, rows // 2)

    def greet(self):
        barrier = pltpu.get_barrier_semaphore()
        for d in (0, 1):
            pl.semaphore_signal(barrier, inc=1, device_id={"tp": self.to[d]}, device_id_type=pl.DeviceIdType.MESH)
        pl.semaphore_wait(barrier, 2)

    def copy(self, kind, d, s, src, dst):
        return pltpu.make_async_remote_copy(
            src_ref=src,
            dst_ref=dst,
            send_sem=self.send.at[kind, d, s],
            recv_sem=self.recv.at[kind, d, s],
            device_id={"tp": self.to[d]},
            device_id_type=pl.DeviceIdType.MESH,
        )

    def own(self, d, s):
        return self.copy(0, d, s, self.blocks.at[s, OWN], self.blocks.at[s, (LEFT, RIGHT)[d]])

    def on(self, d, s):
        half = (self.top, self.low)[d]
        return self.copy(1, d, s, self.blocks.at[s, (LEFT, RIGHT)[d], half], self.blocks.at[s, FAR, half])

    def far(self, d, s):
        return self.copy(2, d, s, self.blocks.at[s, FAR, (self.top, self.low)[d]], self.halves.at[d, s])

    def free(self, d, s):
        half = (self.low, self.top)[d]
        return self.copy(3, d, s, self.blocks.at[s, (RIGHT, LEFT)[d], half], self.sums.at[d, s, half])

    def added(self, d, s):
        half = (self.top, self.low)[d]
        return self.copy(4, d, s, self.blocks.at[s, (RIGHT, LEFT)[d], half], self.sums.at[d, s, half])

    def start_own(self, s):
        for d in (0, 1):
            self.own(d, s).start()

    def pass_on(self, s):
        for d in (0, 1):
            self.own(d, s).wait_recv()
            self.on(d, s).start()

    def gathered(self, s):
        for d in (0, 1):
            self.on(d, s).wait_recv()

    def gather_left(self, s):
        for d in (0, 1):
            self.own(d, s).wait_send()
            self.on(d, s).wait_send()

    def start_added(self, s, wait):
        for d, slot in ((0, RIGHT), (1, LEFT)):
            self.far(d, s).wait_recv()
            half = (self.top, self.low)[d]
            self.blocks[s, slot, half, :] = (wait[d] + self.halves[d, s].astype(jnp.float32)).astype(jnp.bfloat16)
            self.added(d, s).start()

    def summed(self, s):
        for d in (0, 1):
            self.free(d, s).wait_recv()
            self.added(d, s).wait_recv()

    def scatter_left(self, s):
        for d in (0, 1):
            self.free(d, s).wait_send()
            self.added(d, s).wait_send()


def _normed(x, gain):
    wide = x.astype(jnp.float32)
    scale = lax.rsqrt(jnp.mean(wide * wide, -1, keepdims=True) + 1e-6)
    return (wide * scale * gain.astype(jnp.float32)).astype(jnp.bfloat16)


def _send_normed(ring, x_ref, gain_ref):
    rows = ring.blocks.shape[2]
    for s in range(PARTS):
        ring.blocks[s, OWN] = _normed(x_ref[s * rows : (s + 1) * rows, :], gain_ref[...])
        if s < 2:
            ring.start_own(s)
    for s in range(2, PARTS):
        ring.pass_on(s - 2)
        ring.start_own(s)


WIDE = 256
SLOTS = 3


def _mlp(h_ref, gain_ref, gate_ref, up_ref, down_ref, y_ref, sums, blocks, halves, mine, wait, hidden, both, down, send, recv, both_sem,
         down_sem, local_sem):
    ring = Ring(blocks, halves, sums, send, recv)
    rows, width = blocks.shape[2], blocks.shape[3]
    tiles, steps = both.shape[0], width // WIDE

    def weight(t, i):
        at = pl.ds(pl.multiple_of(t * 128, 128), 128)
        return pltpu.make_async_copy((gate_ref, up_ref)[i].at[:, at], both.at[t, :, pl.ds(i * 128, 128)], both_sem.at[i, t])

    def down_tile(g):
        at = pl.ds(pl.multiple_of(lax.rem(g, steps) * WIDE, WIDE), WIDE)
        slot = lax.rem(g, SLOTS)
        return pltpu.make_async_copy(down_ref.at[:, at], down.at[slot], down_sem.at[slot])

    ring.greet()

    @pl.loop(0, tiles)
    def _(t):
        weight(t, 0).start()
        weight(t, 1).start()

    for g in range(SLOTS):
        down_tile(g).start()
    _send_normed(ring, h_ref, gain_ref)

    for s in range(PARTS):
        ring.gathered(s)

        @pl.loop(0, tiles)
        def _(t):
            if s == 0:
                weight(t, 0).wait()
                weight(t, 1).wait()
            gu = jnp.dot(blocks[s].reshape(4 * rows, width), both[t], preferred_element_type=jnp.float32)
            gate, up = gu[:, :128], gu[:, 128:]
            hidden[:, pl.ds(pl.multiple_of(t * 128, 128), 128)] = (gate * jax.nn.sigmoid(gate) * up).astype(jnp.bfloat16)

        if s == 1:
            ring.pass_on(3)
        ring.gather_left(s)

        @pl.loop(0, steps)
        def _(n):
            g = s * steps + n
            down_tile(g).wait()
            at = pl.ds(pl.multiple_of(n * WIDE, WIDE), WIDE)
            term = jnp.dot(hidden[...], down[lax.rem(g, SLOTS)], preferred_element_type=jnp.float32)
            half = rows // 2
            own, right, far, left = (term[k * rows : (k + 1) * rows] for k in range(4))
            blocks[s, FAR, :, at] = far.astype(jnp.bfloat16)
            wait[s, 0, :, at] = right[:half]
            blocks[s, RIGHT, half:, at] = right[half:].astype(jnp.bfloat16)
            blocks[s, LEFT, :half, at] = left[:half].astype(jnp.bfloat16)
            wait[s, 1, :, at] = left[half:]
            mine[s, :, at] = own + h_ref[s * rows : (s + 1) * rows, at].astype(jnp.float32)

            @pl.when(g + SLOTS < PARTS * steps)
            def _():
                down_tile(g + SLOTS).start()

        for d in (0, 1):
            ring.far(d, s).start()
        for d in (0, 1):
            ring.free(d, s).start()
        if s == 0:
            ring.pass_on(2)
        if s >= 1:
            ring.start_added(s - 1, wait.at[s - 1])

    def loads(s):
        return [pltpu.make_async_copy(sums.at[d, s], blocks.at[s, (RIGHT, LEFT)[d]], local_sem.at[d, s]) for d in (0, 1)]

    def store(s):
        return pltpu.make_async_copy(blocks.at[s, OWN], y_ref.at[pl.ds(s * rows, rows), :], local_sem.at[2, s])

    for s in range(PARTS):
        if s == 1:
            ring.start_added(PARTS - 1, wait.at[PARTS - 1])
        ring.summed(s)
        ring.scatter_left(s)
        for c in loads(s):
            c.start()
        for c in loads(s):
            c.wait()
        total = mine[s] + blocks[s, RIGHT].astype(jnp.float32) + blocks[s, LEFT].astype(jnp.float32)
        blocks[s, OWN] = total.astype(jnp.bfloat16)
        store(s).start()
    for s in range(PARTS):
        store(s).wait()
        for d in (0, 1):
            ring.far(d, s).wait_send()


def mlp_half(h, gain, w_gate, w_up, w_down):
    tokens, width = h.shape
    units = w_gate.shape[1]
    rows = tokens // PARTS
    anywhere, vmem = pl.BlockSpec(memory_space=pl.ANY), pl.BlockSpec(memory_space=pltpu.VMEM)
    bf16, f32 = jnp.bfloat16, jnp.float32
    y, _ = pl.pallas_call(
        _mlp,
        in_specs=[vmem, vmem, anywhere, anywhere, anywhere],
        out_specs=[anywhere, anywhere],
        out_shape=[jax.ShapeDtypeStruct(h.shape, bf16), jax.ShapeDtypeStruct((2, PARTS, rows, width), bf16)],
        scratch_shapes=[
            pltpu.VMEM((PARTS, 4, rows, width), bf16),
            pltpu.VMEM((2, PARTS, rows // 2, width), bf16),
            pltpu.VMEM((PARTS, rows, width), f32),
            pltpu.VMEM((PARTS, 2, rows // 2, width), f32),
            pltpu.VMEM((4 * rows, units), bf16),
            pltpu.VMEM((units // 128, width, 256), bf16),
            pltpu.VMEM((SLOTS, units, WIDE), bf16),
            pltpu.SemaphoreType.DMA((KINDS, 2, PARTS)),
            pltpu.SemaphoreType.DMA((KINDS, 2, PARTS)),
            pltpu.SemaphoreType.DMA((2, units // 128)),
            pltpu.SemaphoreType.DMA((SLOTS,)),
            pltpu.SemaphoreType.DMA((3, PARTS)),
        ],
        compiler_params=pltpu.CompilerParams(collective_id=1, has_side_effects=True, vmem_limit_bytes=MOST),
        name="mlp_half",
    )(h, gain.reshape(1, -1), w_gate, w_up, w_down)
    return y


def _turned(t, cos, sin):
    wide = t.astype(jnp.float32)
    return (wide * cos + pltpu.roll(wide, HEAD // 2, 1) * sin).astype(jnp.bfloat16)


def _attention(x_ref, gain_ref, cos_ref, sin_ref, wq_ref, wk_ref, wv_ref, wo_ref, h_ref, blocks, halves, sums, wait, weights, wo, queries,
               keys, values, seen, term, mix_s, top_s, send, recv, weight_sem, local_sem):
    ring = Ring(blocks, halves, sums, send, recv)
    rows, width = blocks.shape[2], blocks.shape[3]
    kv, group = queries.shape[0], queries.shape[3]
    shard = PARTS * rows
    half, cols = rows // 2, group * rows
    q_tiles = wq_ref.shape[1] // WIDE
    e = HEAD**-0.5 * LOG2E

    def weight(n):
        if n < q_tiles:
            return pltpu.make_async_copy(wq_ref.at[:, pl.ds(n * WIDE, WIDE)], weights.at[n], weight_sem.at[n])
        return pltpu.make_async_copy((wk_ref, wv_ref)[n - q_tiles], weights.at[n], weight_sem.at[n])

    def weight_out():
        return pltpu.make_async_copy(wo_ref, wo, weight_sem.at[q_tiles + 2])

    ring.greet()
    for n in range(q_tiles + 2):
        weight(n).start()
    weight_out().start()
    _send_normed(ring, x_ref, gain_ref)
    values[:, HEAD:, :] = jnp.ones((kv, values.shape[1] - HEAD, values.shape[2]), jnp.bfloat16)
    for n in range(q_tiles + 2):
        weight(n).wait()
    weight_out().wait()

    @pl.loop(0, PARTS)
    def _(s):
        ring.gathered(s)
        places = [pl.ds(pl.multiple_of(lax.rem(ring.me + k, 4) * shard + s * rows, rows), rows) for k in range(4)]

        def project(n):
            return jnp.dot(blocks[s].reshape(4 * rows, width), weights[n], preferred_element_type=jnp.float32).astype(jnp.bfloat16)

        @pl.loop(0, q_tiles)
        def _(n):
            t = project(n)
            for k in range(4):
                for i in range(WIDE // HEAD):
                    head = n * (WIDE // HEAD) + i
                    piece = t[k * rows : (k + 1) * rows, i * HEAD : (i + 1) * HEAD]
                    queries[lax.div(head, group), s, k, lax.rem(head, group)] = _turned(piece, cos_ref[places[k], :], sin_ref[places[k], :])

        t = project(q_tiles)
        for k in range(4):
            for i in range(kv):
                piece = t[k * rows : (k + 1) * rows, i * HEAD : (i + 1) * HEAD]
                keys[i, places[k], :] = _turned(piece, cos_ref[places[k], :], sin_ref[places[k], :])
        t = project(q_tiles + 1)
        for k in range(4):
            for i in range(kv):
                values[i, :HEAD, places[k]] = t[k * rows : (k + 1) * rows, i * HEAD : (i + 1) * HEAD].T

        @pl.when(s < PARTS - 2)
        def _():
            ring.pass_on(s + 2)

    for s in range(PARTS):
        ring.gather_left(s)

    def attend_part(k, s):
        last = lax.rem(ring.me + k, 4)
        for i in range(kv):
            top_s[i : i + 1, :] = jnp.full((1, cols), NEG, jnp.float32)
            mix_s[i] = jnp.zeros(mix_s.shape[1:], jnp.float32)

        def block(j, masked):
            here = pl.ds(pl.multiple_of(j * shard, shard), shard)
            scores = [_dot(keys[i, here, :], queries[i, s, k].reshape(cols, HEAD), 1, 1) for i in range(kv)]
            if masked:
                place = lax.rem(lax.broadcasted_iota(jnp.int32, (shard, cols), 1), rows) + s * rows
                ok = lax.broadcasted_iota(jnp.int32, (shard, cols), 0) <= place
            soft, keeps = [], []
            for i in range(kv):
                w = jnp.where(ok, scores[i], HIDDEN) if masked else scores[i]
                old = top_s[i : i + 1, :]
                top = jnp.maximum(old, w.max(axis=0, keepdims=True))
                top_s[i : i + 1, :] = top
                soft.append(jnp.exp2((w - top) * e).astype(jnp.bfloat16))
                keeps.append(jnp.exp2((old - top) * e))
            for i in range(kv):
                mix_s[i] = mix_s[i] * keeps[i] + _dot(values[i, :, here], soft[i], 1, 0)

        lax.fori_loop(0, last, lambda j, _: block(j, False), None)
        block(last, True)
        for i in range(kv):
            out = (mix_s[i, :HEAD, :] * (1 / mix_s[i, HEAD : HEAD + 1, :])).T.astype(jnp.bfloat16)
            for n in range(group):
                at = (i * group + n) * HEAD
                seen[:, at : at + HEAD] = out[n * rows : (n + 1) * rows]

        @pl.loop(0, width // WIDE)
        def _(n):
            at = pl.ds(pl.multiple_of(n * WIDE, WIDE), WIDE)
            term[:, at] = jnp.dot(seen[...], wo[:, at], preferred_element_type=jnp.float32)

    @pl.loop(0, 3 * (PARTS + 1))
    def _(j):
        m, r = lax.div(j, 3), lax.rem(j, 3)
        s = jnp.where(r == 0, m, m - 1)

        @pl.when((s >= 0) & (s < PARTS))
        def _():
            attend_part(jnp.where(r == 0, FAR, jnp.where(r == 1, RIGHT, LEFT)), s)

            @pl.when(r == 0)
            def _():
                blocks[s, FAR] = term[...].astype(jnp.bfloat16)
                for d in (0, 1):
                    ring.far(d, s).start()

            @pl.when(r == 1)
            def _():
                wait[s, 0] = term[:half, :]
                blocks[s, RIGHT, half:, :] = term[half:, :].astype(jnp.bfloat16)
                ring.free(0, s).start()

            @pl.when(r == 2)
            def _():
                wait[s, 1] = term[half:, :]
                blocks[s, LEFT, :half, :] = term[:half, :].astype(jnp.bfloat16)
                ring.free(1, s).start()

                @pl.when(s >= 1)
                def _():
                    ring.start_added(s - 1, wait.at[s - 1])

    def store(s):
        return pltpu.make_async_copy(blocks.at[s, OWN], h_ref.at[pl.ds(pl.multiple_of(s * rows, rows), rows), :], local_sem.at[s])

    @pl.loop(0, PARTS)
    def _(s):
        attend_part(OWN, s)

        @pl.when(s == 0)
        def _():
            ring.start_added(PARTS - 1, wait.at[PARTS - 1])

        ring.summed(s)
        total = term[...] + sums[0, s].astype(jnp.float32) + sums[1, s].astype(jnp.float32)
        mine = x_ref[pl.ds(pl.multiple_of(s * rows, rows), rows), :].astype(jnp.float32)
        blocks[s, OWN] = (mine + total).astype(jnp.bfloat16)
        store(s).start()

    for s in range(PARTS):
        store(s).wait()
        ring.scatter_left(s)
        for d in (0, 1):
            ring.far(d, s).wait_send()


def attention_half(x, gain, wq, wk, wv, wo):
    tokens, width = x.shape
    rows, all_tokens = tokens // PARTS, tokens * lax.axis_size("tp")
    kv = wk.shape[1] // HEAD
    group = wq.shape[1] // HEAD // kv
    angle = jnp.arange(all_tokens).astype(jnp.float32)[:, None] * THETA ** (-jnp.arange(HEAD // 2, dtype=jnp.float32) / (HEAD // 2))
    cos, sin = jnp.cos(angle), jnp.sin(angle)
    cos, sin = jnp.concatenate([cos, cos], -1), jnp.concatenate([-sin, sin], -1)
    anywhere, vmem = pl.BlockSpec(memory_space=pl.ANY), pl.BlockSpec(memory_space=pltpu.VMEM)
    bf16, f32 = jnp.bfloat16, jnp.float32
    return pl.pallas_call(
        _attention,
        in_specs=[vmem, vmem, vmem, vmem, anywhere, anywhere, anywhere, anywhere],
        out_specs=anywhere,
        out_shape=jax.ShapeDtypeStruct(x.shape, bf16),
        scratch_shapes=[
            pltpu.VMEM((PARTS, 4, rows, width), bf16),
            pltpu.VMEM((2, PARTS, rows // 2, width), bf16),
            pltpu.VMEM((2, PARTS, rows, width), bf16),
            pltpu.VMEM((PARTS, 2, rows // 2, width), f32),
            pltpu.VMEM(((wq.shape[1] + wk.shape[1] + wv.shape[1]) // WIDE, width, WIDE), bf16),
            pltpu.VMEM(wo.shape, bf16),
            pltpu.VMEM((kv, PARTS, 4, group, rows, HEAD), bf16),
            pltpu.VMEM((kv, all_tokens, HEAD), bf16),
            pltpu.VMEM((kv, HEAD + 16, all_tokens), bf16),
            pltpu.VMEM((rows, wo.shape[0]), bf16),
            pltpu.VMEM((rows, width), f32),
            pltpu.VMEM((kv, HEAD + 16, group * rows), f32),
            pltpu.VMEM((kv, group * rows), f32),
            pltpu.SemaphoreType.DMA((KINDS, 2, PARTS)),
            pltpu.SemaphoreType.DMA((KINDS, 2, PARTS)),
            pltpu.SemaphoreType.DMA((wq.shape[1] // WIDE + 3,)),
            pltpu.SemaphoreType.DMA((PARTS,)),
        ],
        compiler_params=pltpu.CompilerParams(collective_id=0, has_side_effects=True, vmem_limit_bytes=MOST),
        name="attention_half",
    )(x, gain.reshape(1, -1), cos, sin, wq, wk, wv, wo)


def solution(mesh):
    def step(x, gain_a, wq, wk, wv, wo, gain_m, w_gate, w_up, w_down):
        h = attention_half(x, gain_a, wq, wk, wv, wo)
        return mlp_half(h, gain_m, w_gate, w_up, w_down)

    tokens, columns, rows_of = P(("dp", "tp"), None), P(None, "tp"), P("tp", None)
    return jax.shard_map(
        step,
        mesh=mesh,
        in_specs=(tokens, P(None), columns, columns, columns, rows_of, P(None), columns, columns, rows_of),
        out_specs=tokens,
        check_vma=False,
    )
```

```python
import jax
import jax.numpy as jnp
import numpy as np
from jax import lax
from jax.experimental import pallas as pl
from jax.experimental.pallas import tpu as pltpu

NEG = -1e30
HIDDEN = 2 * NEG
LOG2E = 1.4426950408889634


def _dot(a, b, ca, cb):
    return lax.dot_general(a, b, (((ca,), (cb,)), ((), ())), preferred_element_type=jnp.float32)


from jax.sharding import PartitionSpec as P

HEAD = 128
THETA = 10000
LEFT, OWN, RIGHT, FAR = 0, 1, 2, 3
PARTS = 4
MOST = 67_043_328
KINDS = 5
WIDE = 256
SLOTS = 3


class Ring:
    def __init__(self, trip, blocks, halves, sums, send, recv):
        self.blocks, self.halves, self.sums, self.send, self.recv = blocks, halves, sums, send, recv
        self.trip = trip
        n = lax.axis_size("tp")
        self.me = lax.axis_index("tp")
        self.to = (lax.rem(self.me + 1, n), lax.rem(self.me + n - 1, n))
        rows = blocks.shape[2]
        self.top, self.low = pl.ds(0, rows // 2), pl.ds(rows // 2, rows // 2)

    def greet(self):
        barrier = pltpu.get_barrier_semaphore()
        for d in (0, 1):
            pl.semaphore_signal(barrier, inc=1, device_id={"tp": self.to[d]}, device_id_type=pl.DeviceIdType.MESH)
        pl.semaphore_wait(barrier, 2)

    def copy(self, kind, d, s, src, dst):
        return pltpu.make_async_remote_copy(
            src_ref=src,
            dst_ref=dst,
            send_sem=self.send.at[self.trip, kind, d, s],
            recv_sem=self.recv.at[self.trip, kind, d, s],
            device_id={"tp": self.to[d]},
            device_id_type=pl.DeviceIdType.MESH,
        )

    def own(self, d, s):
        return self.copy(0, d, s, self.blocks.at[s, OWN], self.blocks.at[s, (LEFT, RIGHT)[d]])

    def on(self, d, s):
        half = (self.top, self.low)[d]
        return self.copy(1, d, s, self.blocks.at[s, (LEFT, RIGHT)[d], half], self.blocks.at[s, FAR, half])

    def far(self, d, s):
        return self.copy(2, d, s, self.blocks.at[s, FAR, (self.top, self.low)[d]], self.halves.at[d, s])

    def free(self, d, s):
        half = (self.low, self.top)[d]
        return self.copy(3, d, s, self.blocks.at[s, (RIGHT, LEFT)[d], half], self.sums.at[d, s, half])

    def added(self, d, s):
        half = (self.top, self.low)[d]
        return self.copy(4, d, s, self.blocks.at[s, (RIGHT, LEFT)[d], half], self.sums.at[d, s, half])

    def start_own(self, s):
        for d in (0, 1):
            self.own(d, s).start()

    def pass_on(self, s):
        for d in (0, 1):
            self.own(d, s).wait_recv()
            self.on(d, s).start()

    def gathered(self, s):
        for d in (0, 1):
            self.on(d, s).wait_recv()

    def gather_left(self, s):
        for d in (0, 1):
            self.own(d, s).wait_send()
            self.on(d, s).wait_send()

    def start_added(self, s, wait):
        for d, slot in ((0, RIGHT), (1, LEFT)):
            self.far(d, s).wait_recv()
            half = (self.top, self.low)[d]
            self.blocks[s, slot, half, :] = (wait[d] + self.halves[d, s].astype(jnp.float32)).astype(jnp.bfloat16)
            self.added(d, s).start()

    def give(self, credit, s):
        self.scatter_left(s)
        for d in (0, 1):
            pl.semaphore_signal(credit.at[d, s], inc=1, device_id={"tp": self.to[d]}, device_id_type=pl.DeviceIdType.MESH)

    def take(self, credit, s):
        for d in (0, 1):
            pl.semaphore_wait(credit.at[d, s], 1)

    def summed(self, s):
        for d in (0, 1):
            self.free(d, s).wait_recv()
            self.added(d, s).wait_recv()

    def scatter_left(self, s):
        for d in (0, 1):
            self.far(d, s).wait_send()
            self.free(d, s).wait_send()
            self.added(d, s).wait_send()


def _normed(wide, gain_ref):
    scale = lax.rsqrt(jnp.mean(wide * wide, -1, keepdims=True) + 1e-6)
    return (wide * scale * gain_ref[...].reshape(1, -1).astype(jnp.float32)).astype(jnp.bfloat16)


def _turned(t, cos, sin):
    wide = t.astype(jnp.float32)
    return (wide * cos + pltpu.roll(wide, HEAD // 2, 1) * sin).astype(jnp.bfloat16)


def _layer(x_ref, gain_a, turn_ref, wq_ref, wk_ref, wv_ref, wo_ref, gain_m, gate_ref, up_ref, down_ref, y_ref, blocks, halves, sums, wait, mine,
           send, recv, weight_sem, both_sem, down_sem, local_sem,
           credit):
    rows, width = blocks.shape[2], blocks.shape[3]
    shard, half = PARTS * rows, rows // 2
    ring = Ring(0, blocks, halves, sums, send, recv)
    bf16, f32 = jnp.bfloat16, jnp.float32
    kv = wk_ref.shape[1] // HEAD
    group = wq_ref.shape[1] // HEAD // kv
    tokens = 4 * shard
    q_tiles = wq_ref.shape[1] // WIDE
    units = gate_ref.shape[1]

    def span(i, size):
        return pl.ds(pl.multiple_of(i * size, size), size)

    def load(s):
        return pltpu.make_async_copy(x_ref.at[span(s, rows), :], blocks.at[s, OWN], local_sem.at[s])

    def store(s):
        return pltpu.make_async_copy(blocks.at[s, OWN], y_ref.at[span(s, rows), :], local_sem.at[s])

    def attention(weights, wo, queries, keys, values, cos_s, sin_s, seen, term, mix_s, top_s):
        cols = group * rows
        e = HEAD**-0.5 * LOG2E

        def weight(n):
            source = wq_ref.at[:, pl.ds(n * WIDE, WIDE)] if n < q_tiles else (wk_ref, wv_ref)[n - q_tiles]
            return pltpu.make_async_copy(source, weights.at[n], weight_sem.at[n])

        def weight_out():
            return pltpu.make_async_copy(wo_ref, wo, weight_sem.at[q_tiles + 2])

        for s in range(PARTS):
            load(s).start()
        ring.greet()
        for s in range(PARTS):
            load(s).wait()
            wide = blocks[s, OWN].astype(f32)
            mine[s] = wide
            blocks[s, OWN] = _normed(wide, gain_a)
            if s < 2:
                ring.start_own(s)
            if s == 1:
                for n in range(q_tiles + 2):
                    weight(n).start()
                weight_out().start()

        @pl.loop(0, tokens // shard)
        def _(i):
            at = span(i, shard)
            angle = (lax.broadcasted_iota(jnp.int32, (shard, HEAD), 0) + i * shard).astype(f32) * turn_ref[...]
            cos_s[at, :] = jnp.cos(angle)
            sine = jnp.sin(angle)
            sin_s[at, :] = jnp.where(lax.broadcasted_iota(jnp.int32, (shard, HEAD), 1) < HEAD // 2, -sine, sine)

        keys[...] = jnp.zeros(keys.shape, bf16)
        values[:, :HEAD, :] = jnp.zeros((kv, HEAD, tokens), bf16)
        values[:, HEAD:, :] = jnp.ones((kv, values.shape[1] - HEAD, tokens), bf16)
        for n in range(q_tiles + 2):
            weight(n).wait()

        def project(s, first, count):
            places = [pl.ds(pl.multiple_of(lax.rem(ring.me + k + 3, 4) * shard + s * rows, rows), rows) for k in range(first, first + count)]

            def tile(n):
                rows_of = blocks[s, first : first + count].reshape(count * rows, width)
                return jnp.dot(rows_of, weights[n], preferred_element_type=f32).astype(bf16)

            def piece(t, k, i):
                return t[k * rows : (k + 1) * rows, i * HEAD : (i + 1) * HEAD]

            @pl.loop(0, q_tiles)
            def _(n):
                t = tile(n)
                for k in range(count):
                    for i in range(WIDE // HEAD):
                        head = n * (WIDE // HEAD) + i
                        turned = _turned(piece(t, k, i), cos_s[places[k], :], sin_s[places[k], :])
                        queries[lax.div(head, group), s, first + k, lax.rem(head, group)] = turned

            t = tile(q_tiles)
            for k in range(count):
                for i in range(kv):
                    keys[i, places[k], :] = _turned(piece(t, k, i), cos_s[places[k], :], sin_s[places[k], :])
            t = tile(q_tiles + 1)
            for k in range(count):
                for i in range(kv):
                    values[i, :HEAD, places[k]] = piece(t, k, i).T

        @pl.loop(0, PARTS)
        def _(s):
            ring.pass_on(s)

            @pl.when(s < PARTS - 2)
            def _():
                ring.start_own(s + 2)

            project(s, LEFT, 3)

            @pl.when((s >= 1) & (s < PARTS - 1))
            def _():
                ring.gathered(s - 1)
                project(s - 1, FAR, 1)

        weight_out().wait()

        def attend_part(k, s):
            last = lax.rem(ring.me + k + 3, 4)
            for i in range(kv):
                top_s[i : i + 1, :] = jnp.full((1, cols), NEG, f32)
                mix_s[i] = jnp.zeros(mix_s.shape[1:], f32)

            def block(j, masked):
                here = span(j, shard)
                scores = [_dot(keys[i, here, :], queries[i, s, k].reshape(cols, HEAD), 1, 1) for i in range(kv)]
                if masked:
                    place = lax.rem(lax.broadcasted_iota(jnp.int32, (shard, cols), 1), rows) + s * rows
                    ok = lax.broadcasted_iota(jnp.int32, (shard, cols), 0) <= place
                soft, keeps = [], []
                for i in range(kv):
                    w = jnp.where(ok, scores[i], HIDDEN) if masked else scores[i]
                    old = top_s[i : i + 1, :]
                    top = jnp.maximum(old, w.max(axis=0, keepdims=True))
                    top_s[i : i + 1, :] = top
                    soft.append(jnp.exp2((w - top) * e).astype(bf16))
                    keeps.append(jnp.exp2((old - top) * e))
                for i in range(kv):
                    mix_s[i] = mix_s[i] * keeps[i] + _dot(values[i, :, here], soft[i], 1, 0)

            lax.fori_loop(0, last, lambda j, _: block(j, False), None)
            block(last, True)
            for i in range(kv):
                out = (mix_s[i, :HEAD, :] * (1 / mix_s[i, HEAD : HEAD + 1, :])).T.astype(bf16)
                for n in range(group):
                    at = (i * group + n) * HEAD
                    seen[:, at : at + HEAD] = out[n * rows : (n + 1) * rows]

            @pl.loop(0, width // WIDE)
            def _(n):
                at = span(n, WIDE)
                term[:, at] = jnp.dot(seen[...], wo[:, at], preferred_element_type=f32)

        @pl.loop(0, 2 + 3 * PARTS)
        def _(j):
            m, r = lax.div(j - 2, 3), lax.rem(j - 2, 3)
            early = j < 2
            kind = jnp.where(early, 0, r)
            s = jnp.where(early, j, jnp.where(r == 0, m + 2, m))

            @pl.when(s < PARTS)
            def _():
                attend_part(jnp.where(kind == 0, FAR, jnp.where(kind == 1, RIGHT, LEFT)), s)

                @pl.when(kind == 0)
                def _():
                    blocks[s, FAR] = term[...].astype(bf16)
                    for d in (0, 1):
                        ring.far(d, s).start()

                @pl.when(kind == 1)
                def _():
                    wait[s, 0] = term[:half, :]
                    blocks[s, RIGHT, half:, :] = term[half:, :].astype(bf16)
                    ring.free(0, s).start()

                @pl.when(kind == 2)
                def _():
                    wait[s, 1] = term[half:, :]
                    blocks[s, LEFT, :half, :] = term[:half, :].astype(bf16)
                    ring.free(1, s).start()

                    @pl.when(s < PARTS - 1)
                    def _():
                        ring.start_added(s, wait.at[s])

            @pl.when(early)
            def _():
                ring.gathered(j + 2)
                project(j + 2, FAR, 1)

            @pl.when(j == 1)
            def _():
                for p in range(PARTS):
                    ring.gather_left(p)

        @pl.loop(0, PARTS)
        def _(s):
            attend_part(OWN, s)
            mine[s] = mine[s] + term[...]

            @pl.when(s == 0)
            def _():
                ring.start_added(PARTS - 1, wait.at[PARTS - 1])

    pl.run_scoped(
        attention,
        pltpu.VMEM((q_tiles + 2, width, WIDE), bf16),
        pltpu.VMEM(wo_ref.shape, bf16),
        pltpu.VMEM((kv, PARTS, 4, group, rows, HEAD), bf16),
        pltpu.VMEM((kv, tokens, HEAD), bf16),
        pltpu.VMEM((kv, HEAD + 16, tokens), bf16),
        pltpu.VMEM((tokens, HEAD), f32),
        pltpu.VMEM((tokens, HEAD), f32),
        pltpu.VMEM((rows, wo_ref.shape[0]), bf16),
        pltpu.VMEM((rows, width), f32),
        pltpu.VMEM((kv, HEAD + 16, group * rows), f32),
        pltpu.VMEM((kv, group * rows), f32),
    )

    def mlp(hidden, both, down):
        ring = Ring(1, blocks, halves, sums, send, recv)
        tiles, steps = both.shape[0], width // WIDE

        def weight(t, i):
            return pltpu.make_async_copy((gate_ref, up_ref)[i].at[:, span(t, 128)], both.at[t, :, pl.ds(i * 128, 128)], both_sem.at[i, t])

        def down_tile(g):
            slot = lax.rem(g, SLOTS)
            return pltpu.make_async_copy(down_ref.at[:, span(lax.rem(g, steps), WIDE)], down.at[slot], down_sem.at[slot])

        @pl.loop(0, tiles)
        def _(t):
            weight(t, 0).start()
            weight(t, 1).start()

        for g in range(SLOTS):
            down_tile(g).start()

        def finish(s):
            before = Ring(0, blocks, halves, sums, send, recv)
            before.summed(s)
            before.give(credit, s)
            h = (mine[s] + sums[0, s].astype(f32) + sums[1, s].astype(f32)).astype(bf16).astype(f32)
            mine[s] = h
            blocks[s, OWN] = _normed(h, gain_m)

        for s in range(PARTS):
            finish(s)
            if s < 2:
                ring.take(credit, s)
                ring.start_own(s)
        for s in range(2, PARTS):
            ring.pass_on(s - 2)
            ring.take(credit, s)
            ring.start_own(s)

        for s in range(PARTS):
            ring.gathered(s)

            @pl.loop(0, tiles)
            def _(t):
                if s == 0:
                    weight(t, 0).wait()
                    weight(t, 1).wait()
                gu = jnp.dot(blocks[s].reshape(4 * rows, width), both[t], preferred_element_type=f32)
                gate, up = gu[:, :128], gu[:, 128:]
                hidden[:, span(t, 128)] = (gate * jax.nn.sigmoid(gate) * up).astype(bf16)

            if s == 1:
                ring.pass_on(3)
            ring.gather_left(s)

            @pl.loop(0, steps)
            def _(n):
                g = s * steps + n
                down_tile(g).wait()
                at = span(n, WIDE)
                out = jnp.dot(hidden[...], down[lax.rem(g, SLOTS)], preferred_element_type=f32)
                left, own, right, far = (out[k * rows : (k + 1) * rows] for k in range(4))
                blocks[s, FAR, :, at] = far.astype(bf16)
                wait[s, 0, :, at] = right[:half]
                blocks[s, RIGHT, half:, at] = right[half:].astype(bf16)
                blocks[s, LEFT, :half, at] = left[:half].astype(bf16)
                wait[s, 1, :, at] = left[half:]
                mine[s, :, at] = mine[s, :, at] + own

                @pl.when(g + SLOTS < PARTS * steps)
                def _():
                    down_tile(g + SLOTS).start()

            for d in (0, 1):
                ring.far(d, s).start()
            for d in (0, 1):
                ring.free(d, s).start()
            if s == 0:
                ring.pass_on(2)
            if s >= 1:
                ring.start_added(s - 1, wait.at[s - 1])

        for s in range(PARTS):
            if s == 1:
                ring.start_added(PARTS - 1, wait.at[PARTS - 1])
            ring.summed(s)
            blocks[s, OWN] = (mine[s] + sums[0, s].astype(f32) + sums[1, s].astype(f32)).astype(bf16)
            store(s).start()
        for s in range(PARTS):
            store(s).wait()
            ring.scatter_left(s)

    pl.run_scoped(
        mlp,
        pltpu.VMEM((4 * rows, units), bf16),
        pltpu.VMEM((units // 128, width, 256), bf16),
        pltpu.VMEM((SLOTS, units, WIDE), bf16),
    )


def layer(x, gain_a, wq, wk, wv, wo, gain_m, w_gate, w_up, w_down):
    tokens, width = x.shape
    rows, units = tokens // PARTS, w_gate.shape[1]
    turn = (float(THETA) ** (-np.arange(HEAD // 2) / (HEAD // 2))).astype(np.float32)
    turn = jnp.asarray(np.concatenate([turn, turn])[None])
    anywhere, vmem = pl.BlockSpec(memory_space=pl.ANY), pl.BlockSpec(memory_space=pltpu.VMEM)
    bf16, f32 = jnp.bfloat16, jnp.float32
    return pl.pallas_call(
        _layer,
        in_specs=[anywhere, vmem, vmem, anywhere, anywhere, anywhere, anywhere, vmem, anywhere, anywhere, anywhere],
        out_specs=anywhere,
        out_shape=jax.ShapeDtypeStruct(x.shape, bf16),
        scratch_shapes=[
            pltpu.VMEM((PARTS, 4, rows, width), bf16),
            pltpu.VMEM((2, PARTS, rows // 2, width), bf16),
            pltpu.VMEM((2, PARTS, rows, width), bf16),
            pltpu.VMEM((PARTS, 2, rows // 2, width), f32),
            pltpu.VMEM((PARTS, rows, width), f32),
            pltpu.SemaphoreType.DMA((2, KINDS, 2, PARTS)),
            pltpu.SemaphoreType.DMA((2, KINDS, 2, PARTS)),
            pltpu.SemaphoreType.DMA((wq.shape[1] // WIDE + 3,)),
            pltpu.SemaphoreType.DMA((2, units // 128)),
            pltpu.SemaphoreType.DMA((SLOTS,)),
            pltpu.SemaphoreType.DMA((PARTS,)),
            pltpu.SemaphoreType.REGULAR((2, PARTS)),
        ],
        compiler_params=pltpu.CompilerParams(collective_id=0, has_side_effects=True, vmem_limit_bytes=MOST),
        name="layer",
    )(x, gain_a, turn, wq, wk, wv, wo, gain_m, w_gate, w_up, w_down)


def solution(mesh):
    tokens, columns, rows_of = P(("dp", "tp"), None), P(None, "tp"), P("tp", None)
    return jax.shard_map(
        layer,
        mesh=mesh,
        in_specs=(tokens, P(None), columns, columns, columns, rows_of, P(None), columns, columns, rows_of),
        out_specs=tokens,
        check_vma=False,
    )
```

```python
import jax
import jax.numpy as jnp
import numpy as np
from jax import lax
from jax.experimental import pallas as pl
from jax.experimental.pallas import tpu as pltpu

NEG = -1e30
HIDDEN = 2 * NEG
LOG2E = 1.4426950408889634


def _dot(a, b, ca, cb):
    return lax.dot_general(a, b, (((ca,), (cb,)), ((), ())), preferred_element_type=jnp.float32)


from jax.sharding import PartitionSpec as P

HEAD = 128
THETA = 10000
LEFT, OWN, RIGHT, FAR = 0, 1, 2, 3
PARTS = 4
MOST = 67_043_328
KINDS = 5
WIDE = 256
SLOTS = 4
GATE_STEP, DOWN_STEP = 2, 2


class Ring:
    def __init__(self, trip, blocks, halves, sums, send, recv):
        self.blocks, self.halves, self.sums, self.send, self.recv = blocks, halves, sums, send, recv
        self.trip = trip
        n = lax.axis_size("tp")
        self.me = lax.axis_index("tp")
        self.to = (lax.rem(self.me + 1, n), lax.rem(self.me + n - 1, n))
        rows = blocks.shape[2]
        self.top, self.low = pl.ds(0, rows // 2), pl.ds(rows // 2, rows // 2)

    def greet(self):
        barrier = pltpu.get_barrier_semaphore()
        for d in (0, 1):
            pl.semaphore_signal(barrier, inc=1, device_id={"tp": self.to[d]}, device_id_type=pl.DeviceIdType.MESH)

    def met(self):
        pl.semaphore_wait(pltpu.get_barrier_semaphore(), 2)

    def copy(self, kind, d, s, src, dst):
        return pltpu.make_async_remote_copy(
            src_ref=src,
            dst_ref=dst,
            send_sem=self.send.at[self.trip, kind, d, s],
            recv_sem=self.recv.at[self.trip, kind, d, s],
            device_id={"tp": self.to[d]},
            device_id_type=pl.DeviceIdType.MESH,
        )

    def own(self, d, s):
        return self.copy(0, d, s, self.blocks.at[s, OWN], self.blocks.at[s, (LEFT, RIGHT)[d]])

    def on(self, d, s):
        half = (self.top, self.low)[d]
        return self.copy(1, d, s, self.blocks.at[s, (LEFT, RIGHT)[d], half], self.blocks.at[s, FAR, half])

    def far(self, d, s):
        return self.copy(2, d, s, self.blocks.at[s, FAR, (self.top, self.low)[d]], self.halves.at[d, s])

    def free(self, d, s):
        half = (self.low, self.top)[d]
        return self.copy(3, d, s, self.blocks.at[s, (RIGHT, LEFT)[d], half], self.sums.at[d, s, half])

    def added(self, d, s):
        half = (self.top, self.low)[d]
        return self.copy(4, d, s, self.blocks.at[s, (RIGHT, LEFT)[d], half], self.sums.at[d, s, half])

    def start_own(self, s):
        for d in (0, 1):
            self.own(d, s).start()

    def pass_on(self, s):
        for d in (0, 1):
            self.own(d, s).wait_recv()
            self.on(d, s).start()

    def gathered(self, s):
        for d in (0, 1):
            self.on(d, s).wait_recv()

    def gather_left(self, s):
        for d in (0, 1):
            self.own(d, s).wait_send()
            self.on(d, s).wait_send()

    def start_added(self, s, wait):
        for d, slot in ((0, RIGHT), (1, LEFT)):
            self.far(d, s).wait_recv()
            half = (self.top, self.low)[d]
            self.blocks[s, slot, half, :] = (wait[d] + self.halves[d, s].astype(jnp.float32)).astype(jnp.bfloat16)
            self.added(d, s).start()

    def give(self, credit, s):
        self.scatter_left(s)
        for d in (0, 1):
            pl.semaphore_signal(credit.at[d, s], inc=1, device_id={"tp": self.to[d]}, device_id_type=pl.DeviceIdType.MESH)

    def take(self, credit, s):
        for d in (0, 1):
            pl.semaphore_wait(credit.at[d, s], 1)

    def summed(self, s):
        for d in (0, 1):
            self.free(d, s).wait_recv()
            self.added(d, s).wait_recv()

    def scatter_left(self, s):
        for d in (0, 1):
            self.far(d, s).wait_send()
            self.free(d, s).wait_send()
            self.added(d, s).wait_send()


def _steps(n, by, body, before=None, after=None):
    def step(ts):
        for f in (before, body, after):
            for t in ts:
                if f is not None:
                    f(t)

    pl.loop(0, n // by)(lambda i: step([i * by + u for u in range(by)]))
    if n % by:
        step(range(n - n % by, n))


def _normed(wide, gain_ref):
    scale = lax.rsqrt(jnp.mean(wide * wide, -1, keepdims=True) + 1e-6)
    return (wide * scale * gain_ref[...].reshape(1, -1).astype(jnp.float32)).astype(jnp.bfloat16)


def _turned(t, cos, sin):
    wide = t.astype(jnp.float32)
    return (wide * cos + pltpu.roll(wide, HEAD // 2, 1) * sin).astype(jnp.bfloat16)


def _layer(x_ref, gain_a, turn_ref, wq_ref, wk_ref, wv_ref, wo_ref, gain_m, gate_ref, up_ref, down_ref, y_ref, blocks, halves, sums, wait, mine,
           send, recv, weight_sem, both_sem, down_sem, local_sem,
           credit):
    rows, width = blocks.shape[2], blocks.shape[3]
    shard, half = PARTS * rows, rows // 2
    ring = Ring(0, blocks, halves, sums, send, recv)
    bf16, f32 = jnp.bfloat16, jnp.float32
    kv = wk_ref.shape[1] // HEAD
    group = wq_ref.shape[1] // HEAD // kv
    tokens = 4 * shard
    q_tiles = wq_ref.shape[1] // WIDE
    units = gate_ref.shape[1]

    def span(i, size):
        return pl.ds(pl.multiple_of(i * size, size), size)

    def load(s):
        return pltpu.make_async_copy(x_ref.at[span(s, rows), :], blocks.at[s, OWN], local_sem.at[s])

    def store(s):
        return pltpu.make_async_copy(blocks.at[s, OWN], y_ref.at[span(s, rows), :], local_sem.at[s])

    def attention(weights, wo, queries, keys, values, cos_s, sin_s, seen, term, mix_s, top_s):
        cols = group * rows
        e = HEAD**-0.5 * LOG2E

        def weight(n):
            source = wq_ref.at[:, pl.ds(n * WIDE, WIDE)] if n < q_tiles else (wk_ref, wv_ref)[n - q_tiles]
            return pltpu.make_async_copy(source, weights.at[n], weight_sem.at[n])

        def weight_out():
            return pltpu.make_async_copy(wo_ref, wo, weight_sem.at[q_tiles + 2])

        ring.greet()
        for s in range(PARTS):
            load(s).start()
        for s in range(PARTS):
            load(s).wait()
            wide = blocks[s, OWN].astype(f32)
            mine[s] = wide
            blocks[s, OWN] = _normed(wide, gain_a)
            if s == 0:
                ring.met()
            if s < 2:
                ring.start_own(s)
            if s == 1:
                for n in range(q_tiles + 2):
                    weight(n).start()
                weight_out().start()

        @pl.loop(0, tokens // shard)
        def _(i):
            at = span(i, shard)
            angle = (lax.broadcasted_iota(jnp.int32, (shard, HEAD), 0) + i * shard).astype(f32) * turn_ref[...]
            cos_s[at, :] = jnp.cos(angle)
            sine = jnp.sin(angle)
            sin_s[at, :] = jnp.where(lax.broadcasted_iota(jnp.int32, (shard, HEAD), 1) < HEAD // 2, -sine, sine)

        keys[...] = jnp.zeros(keys.shape, bf16)
        values[:, :HEAD, :] = jnp.zeros((kv, HEAD, tokens), bf16)
        values[:, HEAD:, :] = jnp.ones((kv, values.shape[1] - HEAD, tokens), bf16)
        for n in range(q_tiles + 2):
            weight(n).wait()

        def project(s, first, count):
            places = [pl.ds(pl.multiple_of(lax.rem(ring.me + k + 3, 4) * shard + s * rows, rows), rows) for k in range(first, first + count)]

            def tile(n):
                rows_of = blocks[s, first : first + count].reshape(count * rows, width)
                return jnp.dot(rows_of, weights[n], preferred_element_type=f32).astype(bf16)

            def piece(t, k, i):
                return t[k * rows : (k + 1) * rows, i * HEAD : (i + 1) * HEAD]

            @pl.loop(0, q_tiles)
            def _(n):
                t = tile(n)
                for k in range(count):
                    for i in range(WIDE // HEAD):
                        head = n * (WIDE // HEAD) + i
                        turned = _turned(piece(t, k, i), cos_s[places[k], :], sin_s[places[k], :])
                        queries[lax.div(head, group), s, first + k, lax.rem(head, group)] = turned

            t = tile(q_tiles)
            for k in range(count):
                for i in range(kv):
                    keys[i, places[k], :] = _turned(piece(t, k, i), cos_s[places[k], :], sin_s[places[k], :])
            t = tile(q_tiles + 1)
            for k in range(count):
                for i in range(kv):
                    values[i, :HEAD, places[k]] = piece(t, k, i).T

        @pl.loop(0, PARTS)
        def _(s):
            ring.pass_on(s)

            @pl.when(s < PARTS - 2)
            def _():
                ring.start_own(s + 2)

            project(s, LEFT, 3)

            @pl.when((s >= 1) & (s < PARTS - 1))
            def _():
                ring.gathered(s - 1)
                project(s - 1, FAR, 1)

        weight_out().wait()

        def attend_part(k, s):
            last = lax.rem(ring.me + k + 3, 4)
            for i in range(kv):
                top_s[i : i + 1, :] = jnp.full((1, cols), NEG, f32)
                mix_s[i] = jnp.zeros(mix_s.shape[1:], f32)

            def block(j, masked):
                here = span(j, shard)
                scores = [_dot(keys[i, here, :], queries[i, s, k].reshape(cols, HEAD), 1, 1) for i in range(kv)]
                if masked:
                    place = lax.rem(lax.broadcasted_iota(jnp.int32, (shard, cols), 1), rows) + s * rows
                    ok = lax.broadcasted_iota(jnp.int32, (shard, cols), 0) <= place
                soft, keeps = [], []
                for i in range(kv):
                    w = jnp.where(ok, scores[i], HIDDEN) if masked else scores[i]
                    old = top_s[i : i + 1, :]
                    top = jnp.maximum(old, w.max(axis=0, keepdims=True))
                    top_s[i : i + 1, :] = top
                    soft.append(jnp.exp2((w - top) * e).astype(bf16))
                    keeps.append(jnp.exp2((old - top) * e))
                for i in range(kv):
                    mix_s[i] = mix_s[i] * keeps[i] + _dot(values[i, :, here], soft[i], 1, 0)

            lax.fori_loop(0, last, lambda j, _: block(j, False), None)
            block(last, True)
            for i in range(kv):
                out = (mix_s[i, :HEAD, :] * (1 / mix_s[i, HEAD : HEAD + 1, :])).T.astype(bf16)
                for n in range(group):
                    at = (i * group + n) * HEAD
                    seen[:, at : at + HEAD] = out[n * rows : (n + 1) * rows]

            @pl.loop(0, 2)
            def _(n):
                at = span(n, width // 2)
                term[:, at] = jnp.dot(seen[...], wo[:, at], preferred_element_type=f32)

        @pl.loop(0, 2 + 3 * PARTS)
        def _(j):
            m, r = lax.div(j - 2, 3), lax.rem(j - 2, 3)
            early = j < 2
            kind = jnp.where(early, 0, r)
            s = jnp.where(early, j, jnp.where(r == 0, m + 2, m))

            @pl.when(s < PARTS)
            def _():
                attend_part(jnp.where(kind == 0, FAR, jnp.where(kind == 1, RIGHT, LEFT)), s)

                @pl.when(kind == 0)
                def _():
                    blocks[s, FAR] = term[...].astype(bf16)
                    for d in (0, 1):
                        ring.far(d, s).start()

                @pl.when(kind == 1)
                def _():
                    wait[s, 0] = term[:half, :]
                    blocks[s, RIGHT, half:, :] = term[half:, :].astype(bf16)
                    ring.free(0, s).start()

                @pl.when(kind == 2)
                def _():
                    wait[s, 1] = term[half:, :]
                    blocks[s, LEFT, :half, :] = term[:half, :].astype(bf16)
                    ring.free(1, s).start()

                    @pl.when(s < PARTS - 1)
                    def _():
                        ring.start_added(s, wait.at[s])

            @pl.when(early)
            def _():
                ring.gathered(j + 2)
                project(j + 2, FAR, 1)

            @pl.when(j == 1)
            def _():
                for p in range(PARTS):
                    ring.gather_left(p)

        @pl.loop(0, PARTS)
        def _(s):
            attend_part(OWN, s)
            mine[s] = mine[s] + term[...]

            @pl.when(s == 0)
            def _():
                ring.start_added(PARTS - 1, wait.at[PARTS - 1])

    pl.run_scoped(
        attention,
        pltpu.VMEM((q_tiles + 2, width, WIDE), bf16),
        pltpu.VMEM(wo_ref.shape, bf16),
        pltpu.VMEM((kv, PARTS, 4, group, rows, HEAD), bf16),
        pltpu.VMEM((kv, tokens, HEAD), bf16),
        pltpu.VMEM((kv, HEAD + 16, tokens), bf16),
        pltpu.VMEM((tokens, HEAD), f32),
        pltpu.VMEM((tokens, HEAD), f32),
        pltpu.VMEM((rows, wo_ref.shape[0]), bf16),
        pltpu.VMEM((rows, width), f32),
        pltpu.VMEM((kv, HEAD + 16, group * rows), f32),
        pltpu.VMEM((kv, group * rows), f32),
    )

    def mlp(hidden, both, down):
        ring = Ring(1, blocks, halves, sums, send, recv)
        tiles, steps = both.shape[0], width // WIDE

        def weight(t, i):
            return pltpu.make_async_copy((gate_ref, up_ref)[i].at[:, span(t, 128)], both.at[t, :, pl.ds(i * 128, 128)], both_sem.at[i, t])

        def down_tile(g):
            slot = lax.rem(g, SLOTS)
            return pltpu.make_async_copy(down_ref.at[:, span(lax.rem(g, steps), WIDE)], down.at[slot], down_sem.at[slot])

        @pl.loop(0, tiles)
        def _(t):
            weight(t, 0).start()
            weight(t, 1).start()

        for g in range(SLOTS):
            down_tile(g).start()

        def finish(s):
            before = Ring(0, blocks, halves, sums, send, recv)
            before.summed(s)
            before.give(credit, s)
            h = (mine[s] + sums[0, s].astype(f32) + sums[1, s].astype(f32)).astype(bf16).astype(f32)
            mine[s] = h
            blocks[s, OWN] = _normed(h, gain_m)

        for s in range(PARTS):
            finish(s)
            if s < 2:
                ring.take(credit, s)
                ring.start_own(s)
        for s in range(2, PARTS):
            ring.pass_on(s - 2)
            ring.take(credit, s)
            ring.start_own(s)

        for s in range(PARTS):
            ring.gathered(s)

            def gate_up(t):
                gu = jnp.dot(blocks[s].reshape(4 * rows, width), both[t], preferred_element_type=f32)
                gate, up = gu[:, :128], gu[:, 128:]
                hidden[:, span(t, 128)] = (gate * jax.nn.sigmoid(gate) * up).astype(bf16)

            def weights_here(t):
                weight(t, 0).wait()
                weight(t, 1).wait()

            _steps(tiles, GATE_STEP, gate_up, weights_here if s == 0 else None)
            if s == 1:
                ring.pass_on(3)
            ring.gather_left(s)

            def bring_down(n):
                g = s * steps + n
                at = span(n, WIDE)
                out = jnp.dot(hidden[...], down[lax.rem(g, SLOTS)], preferred_element_type=f32)
                left, own, right, far = (out[k * rows : (k + 1) * rows] for k in range(4))
                blocks[s, FAR, :, at] = far.astype(bf16)
                wait[s, 0, :, at] = right[:half]
                blocks[s, RIGHT, half:, at] = right[half:].astype(bf16)
                blocks[s, LEFT, :half, at] = left[:half].astype(bf16)
                wait[s, 1, :, at] = left[half:]
                mine[s, :, at] = mine[s, :, at] + own

            def down_next(n):
                g = s * steps + n

                @pl.when(g + SLOTS < PARTS * steps)
                def _():
                    down_tile(g + SLOTS).start()

            _steps(steps, DOWN_STEP, bring_down, lambda n: down_tile(s * steps + n).wait(), down_next)
            if s == 0:
                ring.pass_on(2)
            for d in (0, 1):
                ring.far(d, s).start()
            for d in (0, 1):
                ring.free(d, s).start()
            if s >= 1:
                ring.start_added(s - 1, wait.at[s - 1])

        for s in range(PARTS):
            if s == 1:
                ring.start_added(PARTS - 1, wait.at[PARTS - 1])
            ring.summed(s)
            blocks[s, OWN] = (mine[s] + sums[0, s].astype(f32) + sums[1, s].astype(f32)).astype(bf16)
            store(s).start()
        for s in range(PARTS):
            store(s).wait()
            ring.scatter_left(s)

    pl.run_scoped(
        mlp,
        pltpu.VMEM((4 * rows, units), bf16),
        pltpu.VMEM((units // 128, width, 256), bf16),
        pltpu.VMEM((SLOTS, units, WIDE), bf16),
    )


def layer(x, gain_a, wq, wk, wv, wo, gain_m, w_gate, w_up, w_down):
    tokens, width = x.shape
    rows, units = tokens // PARTS, w_gate.shape[1]
    turn = (float(THETA) ** (-np.arange(HEAD // 2) / (HEAD // 2))).astype(np.float32)
    turn = jnp.asarray(np.concatenate([turn, turn])[None])
    anywhere, vmem = pl.BlockSpec(memory_space=pl.ANY), pl.BlockSpec(memory_space=pltpu.VMEM)
    bf16, f32 = jnp.bfloat16, jnp.float32
    return pl.pallas_call(
        _layer,
        in_specs=[anywhere, vmem, vmem, anywhere, anywhere, anywhere, anywhere, vmem, anywhere, anywhere, anywhere],
        out_specs=anywhere,
        out_shape=jax.ShapeDtypeStruct(x.shape, bf16),
        scratch_shapes=[
            pltpu.VMEM((PARTS, 4, rows, width), bf16),
            pltpu.VMEM((2, PARTS, rows // 2, width), bf16),
            pltpu.VMEM((2, PARTS, rows, width), bf16),
            pltpu.VMEM((PARTS, 2, rows // 2, width), f32),
            pltpu.VMEM((PARTS, rows, width), f32),
            pltpu.SemaphoreType.DMA((2, KINDS, 2, PARTS)),
            pltpu.SemaphoreType.DMA((2, KINDS, 2, PARTS)),
            pltpu.SemaphoreType.DMA((wq.shape[1] // WIDE + 3,)),
            pltpu.SemaphoreType.DMA((2, units // 128)),
            pltpu.SemaphoreType.DMA((SLOTS,)),
            pltpu.SemaphoreType.DMA((PARTS,)),
            pltpu.SemaphoreType.REGULAR((2, PARTS)),
        ],
        compiler_params=pltpu.CompilerParams(collective_id=0, has_side_effects=True, vmem_limit_bytes=MOST),
        name="layer",
    )(x, gain_a, turn, wq, wk, wv, wo, gain_m, w_gate, w_up, w_down)


def solution(mesh):
    tokens, columns, rows_of = P(("dp", "tp"), None), P(None, "tp"), P("tp", None)
    return jax.shard_map(
        layer,
        mesh=mesh,
        in_specs=(tokens, P(None), columns, columns, columns, rows_of, P(None), columns, columns, rows_of),
        out_specs=tokens,
        check_vma=False,
    )
```

```python
import jax
import jax.numpy as jnp
import numpy as np
from jax import lax
from jax.experimental import pallas as pl
from jax.experimental.pallas import tpu as pltpu

NEG = -1e30
HIDDEN = 2 * NEG
LOG2E = 1.4426950408889634


def _dot(a, b, ca, cb):
    return lax.dot_general(a, b, (((ca,), (cb,)), ((), ())), preferred_element_type=jnp.float32)


from jax.sharding import PartitionSpec as P

HEAD = 128
THETA = 10000
LEFT, OWN, RIGHT, FAR = 0, 1, 2, 3
PARTS = 4
MOST = 64_400_000
WIDE = 256
SLOTS = 4
GATE_STEP, DOWN_STEP = 2, 2


def _wait_for(ref, sem):
    pltpu.make_async_copy(ref, ref, sem).wait()


class Ring:
    def __init__(self, blocks, halves, sums, send, recv):
        self.blocks, self.halves, self.sums, self.send, self.recv = blocks, halves, sums, send, recv
        n = lax.axis_size("tp")
        self.me = lax.axis_index("tp")
        self.to = (lax.rem(self.me + 1, n), lax.rem(self.me + n - 1, n))
        rows = blocks.shape[2]
        self.top, self.low = pl.ds(0, rows // 2), pl.ds(rows // 2, rows // 2)

    def greet(self):
        barrier = pltpu.get_barrier_semaphore()
        for d in (0, 1):
            pl.semaphore_signal(barrier, inc=1, device_id={"tp": self.to[d]}, device_id_type=pl.DeviceIdType.MESH)

    def met(self):
        pl.semaphore_wait(pltpu.get_barrier_semaphore(), 2)

    def copy(self, kind, d, s, src, dst):
        return pltpu.make_async_remote_copy(
            src_ref=src,
            dst_ref=dst,
            send_sem=self.send.at[int(kind > 1), s],
            recv_sem=self.recv.at[min(kind, 3), s],
            device_id={"tp": self.to[d]},
            device_id_type=pl.DeviceIdType.MESH,
        )

    def own(self, d, s):
        return self.copy(0, d, s, self.blocks.at[s, OWN], self.blocks.at[s, (LEFT, RIGHT)[d]])

    def on(self, d, s):
        half = (self.top, self.low)[d]
        return self.copy(1, d, s, self.blocks.at[s, (LEFT, RIGHT)[d], half], self.blocks.at[s, FAR, half])

    def far(self, d, s):
        return self.copy(2, d, s, self.blocks.at[s, FAR, (self.top, self.low)[d]], self.halves.at[d, s])

    def free(self, d, s):
        half = (self.low, self.top)[d]
        return self.copy(3, d, s, self.blocks.at[s, (RIGHT, LEFT)[d], half], self.sums.at[d, s, half])

    def added(self, d, s):
        half = (self.top, self.low)[d]
        return self.copy(4, d, s, self.blocks.at[s, (RIGHT, LEFT)[d], half], self.sums.at[d, s, half])

    def start_own(self, s):
        for d in (0, 1):
            self.own(d, s).start()

    def pass_on(self, s):
        _wait_for(self.blocks.at[s, pl.ds(0, 2)], self.recv.at[0, s])
        for d in (0, 1):
            self.on(d, s).start()

    def gathered(self, s):
        _wait_for(self.blocks.at[s, FAR], self.recv.at[1, s])

    def gather_left(self, s):
        _wait_for(self.blocks.at[s, pl.ds(0, 3)], self.send.at[0, s])

    def start_added(self, s, wait):
        _wait_for(self.blocks.at[s, FAR], self.recv.at[2, s])
        for d, slot in ((0, RIGHT), (1, LEFT)):
            half = (self.top, self.low)[d]
            self.blocks[s, slot, half, :] = (wait[d] + self.halves[d, s].astype(jnp.float32)).astype(jnp.bfloat16)
            self.added(d, s).start()

    def give(self, credit, s):
        self.scatter_left(s)
        for d in (0, 1):
            pl.semaphore_signal(credit.at[d], inc=1, device_id={"tp": self.to[d]}, device_id_type=pl.DeviceIdType.MESH)

    def take(self, credit):
        for d in (0, 1):
            pl.semaphore_wait(credit.at[d], 1)

    def summed(self, s):
        _wait_for(self.blocks.at[s, pl.ds(0, 2)], self.recv.at[3, s])

    def scatter_left(self, s):
        _wait_for(self.blocks.at[s, pl.ds(0, 3)], self.send.at[1, s])


def _steps(n, by, body, before=None, after=None):
    def step(ts):
        for f in (before, body, after):
            for t in ts:
                if f is not None:
                    f(t)

    pl.loop(0, n // by)(lambda i: step([i * by + u for u in range(by)]))
    if n % by:
        step(range(n - n % by, n))


def _normed(wide, gain_ref):
    scale = lax.rsqrt(jnp.mean(wide * wide, -1, keepdims=True) + 1e-6)
    return (wide * scale * gain_ref[...].reshape(1, -1).astype(jnp.float32)).astype(jnp.bfloat16)


def _turned(t, cos, sin):
    wide = t.astype(jnp.float32)
    return (wide * cos + pltpu.roll(wide, HEAD // 2, 1) * sin).astype(jnp.bfloat16)


def _layer(x_ref, gain_a_ref, turn_ref, wq_ref, wk_ref, wv_ref, wo_ref, gain_m_ref, gate_ref, up_ref, down_ref, y_ref, blocks, halves, sums, wait, mine,
           send, recv, weight_sem, down_sem, credit,
           gain_a, gain_m, turn):
    rows, width = blocks.shape[2], blocks.shape[3]
    shard, half = PARTS * rows, rows // 2
    ring = Ring(blocks, halves, sums, send, recv)
    bf16, f32 = jnp.bfloat16, jnp.float32
    kv = wk_ref.shape[1] // HEAD
    group = wq_ref.shape[1] // HEAD // kv
    tokens = 4 * shard
    q_tiles = wq_ref.shape[1] // WIDE
    units = gate_ref.shape[1]

    def span(i, size):
        return pl.ds(pl.multiple_of(i * size, size), size)

    def small(i):
        return pltpu.make_async_copy((gain_a_ref, gain_m_ref, turn_ref)[i], (gain_a, gain_m, turn)[i], weight_sem.at[i])

    def load(s):
        return pltpu.make_async_copy(x_ref.at[span(s, rows), :], blocks.at[s, OWN], down_sem.at[s])

    def attention(weights, wo, queries, keys, values, cos_s, sin_s, seen, term, mix_s, top_s):
        cols = group * rows
        e = HEAD**-0.5 * LOG2E

        def weight(n):
            source = wq_ref.at[:, pl.ds(n * WIDE, WIDE)] if n < q_tiles else (wk_ref, wv_ref)[n - q_tiles]
            return pltpu.make_async_copy(source, weights.at[n], weight_sem.at[0])

        def weight_out():
            return pltpu.make_async_copy(wo_ref, wo, weight_sem.at[1])

        ring.greet()
        for s in range(PARTS):
            load(s).start()
        for i in range(3):
            small(i).start()
        for i in range(3):
            small(i).wait()
        for s in range(PARTS):
            load(s).wait()
            wide = blocks[s, OWN].astype(f32)
            mine[s] = wide
            blocks[s, OWN] = _normed(wide, gain_a)
            if s == 0:
                ring.met()
            if s < 2:
                ring.start_own(s)
            if s == 1:
                for n in range(q_tiles + 2):
                    weight(n).start()
                weight_out().start()

        @pl.loop(0, tokens // shard)
        def _(i):
            at = span(i, shard)
            angle = (lax.broadcasted_iota(jnp.int32, (shard, HEAD), 0) + i * shard).astype(f32) * turn[...]
            cos_s[at, :] = jnp.cos(angle)
            sine = jnp.sin(angle)
            sin_s[at, :] = jnp.where(lax.broadcasted_iota(jnp.int32, (shard, HEAD), 1) < HEAD // 2, -sine, sine)

        keys[...] = jnp.zeros(keys.shape, bf16)
        values[:, :HEAD, :] = jnp.zeros((kv, HEAD, tokens), bf16)
        values[:, HEAD:, :] = jnp.ones((kv, values.shape[1] - HEAD, tokens), bf16)
        _wait_for(weights, weight_sem.at[0])

        def project(s, first, count):
            places = [pl.ds(pl.multiple_of(lax.rem(ring.me + k + 3, 4) * shard + s * rows, rows), rows) for k in range(first, first + count)]

            def tile(n):
                rows_of = blocks[s, first : first + count].reshape(count * rows, width)
                return jnp.dot(rows_of, weights[n], preferred_element_type=f32).astype(bf16)

            def piece(t, k, i):
                return t[k * rows : (k + 1) * rows, i * HEAD : (i + 1) * HEAD]

            @pl.loop(0, q_tiles)
            def _(n):
                t = tile(n)
                for k in range(count):
                    for i in range(WIDE // HEAD):
                        head = n * (WIDE // HEAD) + i
                        turned = _turned(piece(t, k, i), cos_s[places[k], :], sin_s[places[k], :])
                        queries[lax.div(head, group), s, first + k, lax.rem(head, group)] = turned

            t = tile(q_tiles)
            for k in range(count):
                for i in range(kv):
                    keys[i, places[k], :] = _turned(piece(t, k, i), cos_s[places[k], :], sin_s[places[k], :])
            t = tile(q_tiles + 1)
            for k in range(count):
                for i in range(kv):
                    values[i, :HEAD, places[k]] = piece(t, k, i).T

        @pl.loop(0, PARTS)
        def _(s):
            ring.pass_on(s)

            @pl.when(s < PARTS - 2)
            def _():
                ring.start_own(s + 2)

            project(s, LEFT, 3)

            @pl.when((s >= 1) & (s < PARTS - 1))
            def _():
                ring.gathered(s - 1)
                project(s - 1, FAR, 1)

        weight_out().wait()

        def attend_part(k, s):
            last = lax.rem(ring.me + k + 3, 4)
            for i in range(kv):
                top_s[i : i + 1, :] = jnp.full((1, cols), NEG, f32)
                mix_s[i] = jnp.zeros(mix_s.shape[1:], f32)

            def block(j, masked):
                here = span(j, shard)
                scores = [_dot(keys[i, here, :], queries[i, s, k].reshape(cols, HEAD), 1, 1) for i in range(kv)]
                if masked:
                    place = lax.rem(lax.broadcasted_iota(jnp.int32, (shard, cols), 1), rows) + s * rows
                    ok = lax.broadcasted_iota(jnp.int32, (shard, cols), 0) <= place
                soft, keeps = [], []
                for i in range(kv):
                    w = jnp.where(ok, scores[i], HIDDEN) if masked else scores[i]
                    old = top_s[i : i + 1, :]
                    top = jnp.maximum(old, w.max(axis=0, keepdims=True))
                    top_s[i : i + 1, :] = top
                    soft.append(jnp.exp2((w - top) * e).astype(bf16))
                    keeps.append(jnp.exp2((old - top) * e))
                for i in range(kv):
                    mix_s[i] = mix_s[i] * keeps[i] + _dot(values[i, :, here], soft[i], 1, 0)

            lax.fori_loop(0, last, lambda j, _: block(j, False), None)
            block(last, True)
            for i in range(kv):
                out = (mix_s[i, :HEAD, :] * (1 / mix_s[i, HEAD : HEAD + 1, :])).T.astype(bf16)
                for n in range(group):
                    at = (i * group + n) * HEAD
                    seen[:, at : at + HEAD] = out[n * rows : (n + 1) * rows]

            @pl.loop(0, 2)
            def _(n):
                at = span(n, width // 2)
                term[:, at] = jnp.dot(seen[...], wo[:, at], preferred_element_type=f32)

        @pl.loop(0, 2 + 3 * PARTS)
        def _(j):
            m, r = lax.div(j - 2, 3), lax.rem(j - 2, 3)
            early = j < 2
            kind = jnp.where(early, 0, r)
            s = jnp.where(early, j, jnp.where(r == 0, m + 2, m))

            @pl.when(s < PARTS)
            def _():
                attend_part(jnp.where(kind == 0, FAR, jnp.where(kind == 1, RIGHT, LEFT)), s)

                @pl.when(kind == 0)
                def _():
                    blocks[s, FAR] = term[...].astype(bf16)
                    for d in (0, 1):
                        ring.far(d, s).start()

                @pl.when(kind == 1)
                def _():
                    wait[0, 0] = term[:half, :]
                    blocks[s, RIGHT, half:, :] = term[half:, :].astype(bf16)
                    ring.free(0, s).start()

                @pl.when(kind == 2)
                def _():
                    wait[0, 1] = term[half:, :]
                    blocks[s, LEFT, :half, :] = term[:half, :].astype(bf16)
                    ring.free(1, s).start()

                    @pl.when(s < PARTS - 1)
                    def _():
                        ring.start_added(s, wait.at[0])

            @pl.when(early)
            def _():
                ring.gathered(j + 2)
                project(j + 2, FAR, 1)

            @pl.when(j == 1)
            def _():
                for p in range(PARTS):
                    ring.gather_left(p)

        @pl.loop(0, PARTS)
        def _(s):
            attend_part(OWN, s)
            mine[s] = mine[s] + term[...]

            @pl.when(s == 0)
            def _():
                ring.start_added(PARTS - 1, wait.at[0])

    pl.run_scoped(
        attention,
        pltpu.VMEM((q_tiles + 2, width, WIDE), bf16),
        pltpu.VMEM(wo_ref.shape, bf16),
        pltpu.VMEM((kv, PARTS, 4, group, rows, HEAD), bf16),
        pltpu.VMEM((kv, tokens, HEAD), bf16),
        pltpu.VMEM((kv, HEAD + 16, tokens), bf16),
        pltpu.VMEM((tokens, HEAD), f32),
        pltpu.VMEM((tokens, HEAD), f32),
        pltpu.VMEM((rows, wo_ref.shape[0]), bf16),
        pltpu.VMEM((rows, width), f32),
        pltpu.VMEM((kv, HEAD + 16, group * rows), f32),
        pltpu.VMEM((kv, group * rows), f32),
    )

    def mlp(hidden, both, down):
        tiles, steps = both.shape[0], width // WIDE

        def weight(t, i):
            return pltpu.make_async_copy((gate_ref, up_ref)[i].at[:, span(t, 128)], both.at[t, :, pl.ds(i * 128, 128)], weight_sem.at[0])

        def down_tile(g):
            slot = lax.rem(g, SLOTS)
            return pltpu.make_async_copy(down_ref.at[:, span(lax.rem(g, steps), WIDE)], down.at[slot], down_sem.at[slot])

        @pl.loop(0, tiles)
        def _(t):
            weight(t, 0).start()
            weight(t, 1).start()

        for g in range(SLOTS):
            down_tile(g).start()

        def finish(s):
            ring.summed(s)
            ring.give(credit, s)
            h = (mine[s] + sums[0, s].astype(f32) + sums[1, s].astype(f32)).astype(bf16).astype(f32)
            mine[s] = h
            blocks[s, OWN] = _normed(h, gain_m)

        for s in range(PARTS):
            finish(s)
            if s < 2:
                ring.take(credit)
                ring.start_own(s)
        for s in range(2, PARTS):
            ring.pass_on(s - 2)
            ring.take(credit)
            ring.start_own(s)

        for s in range(PARTS):
            ring.gathered(s)

            def gate_up(t):
                gu = jnp.dot(blocks[s].reshape(4 * rows, width), both[t], preferred_element_type=f32)
                gate, up = gu[:, :128], gu[:, 128:]
                hidden[:, span(t, 128)] = (gate * jax.nn.sigmoid(gate) * up).astype(bf16)

            if s == 0:
                _wait_for(both, weight_sem.at[0])
            _steps(tiles, GATE_STEP, gate_up)
            if s == 1:
                ring.pass_on(3)
            ring.gather_left(s)

            def bring_down(n):
                g = s * steps + n
                at = span(n, WIDE)
                out = jnp.dot(hidden[...], down[lax.rem(g, SLOTS)], preferred_element_type=f32)
                left, own, right, far = (out[k * rows : (k + 1) * rows] for k in range(4))
                blocks[s, FAR, :, at] = far.astype(bf16)
                wait[s % 2, 0, :, at] = right[:half]
                blocks[s, RIGHT, half:, at] = right[half:].astype(bf16)
                blocks[s, LEFT, :half, at] = left[:half].astype(bf16)
                wait[s % 2, 1, :, at] = left[half:]
                mine[s, :, at] = mine[s, :, at] + own

            def down_next(n):
                g = s * steps + n

                @pl.when(g + SLOTS < PARTS * steps)
                def _():
                    down_tile(g + SLOTS).start()

            _steps(steps, DOWN_STEP, bring_down, lambda n: down_tile(s * steps + n).wait(), down_next)
            if s == 0:
                ring.pass_on(2)
            for d in (0, 1):
                ring.far(d, s).start()
            for d in (0, 1):
                ring.free(d, s).start()
            if s >= 1:
                ring.start_added(s - 1, wait.at[(s - 1) % 2])

        for s in range(PARTS):
            if s == 1:
                ring.start_added(PARTS - 1, wait.at[(PARTS - 1) % 2])
            ring.summed(s)
            y_ref[s * rows : (s + 1) * rows, :] = (mine[s] + sums[0, s].astype(f32) + sums[1, s].astype(f32)).astype(bf16)
        for s in range(PARTS):
            ring.scatter_left(s)

    pl.run_scoped(
        mlp,
        pltpu.VMEM((4 * rows, units), bf16),
        pltpu.VMEM((units // 128, width, 256), bf16),
        pltpu.VMEM((SLOTS, units, WIDE), bf16),
    )


def layer(x, gain_a, wq, wk, wv, wo, gain_m, w_gate, w_up, w_down):
    tokens, width = x.shape
    rows, units = tokens // PARTS, w_gate.shape[1]
    turn = (float(THETA) ** (-np.arange(HEAD // 2) / (HEAD // 2))).astype(np.float32)
    turn = jnp.asarray(np.concatenate([turn, turn])[None])
    anywhere, vmem = pl.BlockSpec(memory_space=pl.ANY), pl.BlockSpec(memory_space=pltpu.VMEM)
    bf16, f32 = jnp.bfloat16, jnp.float32
    return pl.pallas_call(
        _layer,
        in_specs=[anywhere] * 11,
        out_specs=vmem,
        out_shape=pltpu.VMEM(x.shape, bf16),
        scratch_shapes=[
            pltpu.VMEM((PARTS, 4, rows, width), bf16),
            pltpu.VMEM((2, PARTS, rows // 2, width), bf16),
            pltpu.VMEM((2, PARTS, rows, width), bf16),
            pltpu.VMEM((2, 2, rows // 2, width), f32),
            pltpu.VMEM((PARTS, rows, width), f32),
            pltpu.SemaphoreType.DMA((2, PARTS)),
            pltpu.SemaphoreType.DMA((4, PARTS)),
            pltpu.SemaphoreType.DMA((3,)),
            pltpu.SemaphoreType.DMA((max(SLOTS, PARTS),)),
            pltpu.SemaphoreType.REGULAR((2,)),
            pltpu.VMEM(gain_a.shape, bf16),
            pltpu.VMEM(gain_m.shape, bf16),
            pltpu.VMEM(turn.shape, f32),
        ],
        compiler_params=pltpu.CompilerParams(collective_id=0, has_side_effects=True, vmem_limit_bytes=MOST),
        name="layer",
    )(x, gain_a, turn, wq, wk, wv, wo, gain_m, w_gate, w_up, w_down)


def solution(mesh):
    tokens, columns, rows_of = P(("dp", "tp"), None), P(None, "tp"), P("tp", None)
    return jax.shard_map(
        layer,
        mesh=mesh,
        in_specs=(tokens, P(None), columns, columns, columns, rows_of, P(None), columns, columns, rows_of),
        out_specs=tokens,
        check_vma=False,
    )
```

```python
import jax
import jax.numpy as jnp
import numpy as np
from jax import lax
from jax.experimental import pallas as pl
from jax.experimental.pallas import tpu as pltpu

NEG = -1e30
HIDDEN = 2 * NEG
LOG2E = 1.4426950408889634


def _dot(a, b, ca, cb):
    return lax.dot_general(a, b, (((ca,), (cb,)), ((), ())), preferred_element_type=jnp.float32)


from jax.sharding import PartitionSpec as P

HEAD = 128
THETA = 10000
LEFT, OWN, RIGHT, FAR = 0, 1, 2, 3
PARTS = 4
MOST = 64_400_000
WIDE = 256
SLOTS = 4
GATE_STEP, DOWN_STEP = 2, 2


def _wait_for(ref, sem):
    pltpu.make_async_copy(ref, ref, sem).wait()


class Ring:
    def __init__(self, blocks, halves, sums, send, recv):
        self.blocks, self.halves, self.sums, self.send, self.recv = blocks, halves, sums, send, recv
        n = lax.axis_size("tp")
        self.me = lax.axis_index("tp")
        self.to = (lax.rem(self.me + 1, n), lax.rem(self.me + n - 1, n))
        rows = blocks.shape[2]
        self.top, self.low = pl.ds(0, rows // 2), pl.ds(rows // 2, rows // 2)

    def greet(self):
        barrier = pltpu.get_barrier_semaphore()
        for d in (0, 1):
            pl.semaphore_signal(barrier, inc=1, device_id={"tp": self.to[d]}, device_id_type=pl.DeviceIdType.MESH)

    def met(self):
        pl.semaphore_wait(pltpu.get_barrier_semaphore(), 2)

    def copy(self, kind, d, s, src, dst):
        return pltpu.make_async_remote_copy(
            src_ref=src,
            dst_ref=dst,
            send_sem=self.send.at[int(kind > 1), s],
            recv_sem=self.recv.at[(0, 1, 2, 0, (3, 1)[d])[kind], s],
            device_id={"tp": self.to[d]},
            device_id_type=pl.DeviceIdType.MESH,
        )

    def own(self, d, s):
        return self.copy(0, d, s, self.blocks.at[s, OWN], self.blocks.at[s, (LEFT, RIGHT)[d]])

    def on(self, d, s):
        half = (self.top, self.low)[d]
        return self.copy(1, d, s, self.blocks.at[s, (LEFT, RIGHT)[d], half], self.blocks.at[s, FAR, half])

    def far(self, d, s):
        return self.copy(2, d, s, self.blocks.at[s, FAR, (self.top, self.low)[d]], self.halves.at[d, s])

    def free(self, d, s):
        half = (self.low, self.top)[d]
        return self.copy(3, d, s, self.blocks.at[s, (RIGHT, LEFT)[d], half], self.sums.at[d, s, half])

    def added(self, d, s):
        half = (self.top, self.low)[d]
        return self.copy(4, d, s, self.blocks.at[s, (RIGHT, LEFT)[d], half], self.sums.at[d, s, half])

    def start_own(self, s):
        for d in (0, 1):
            self.own(d, s).start()

    def pass_on(self, s):
        _wait_for(self.blocks.at[s, pl.ds(0, 2)], self.recv.at[0, s])
        for d in (0, 1):
            self.on(d, s).start()

    def gathered(self, s):
        _wait_for(self.blocks.at[s, FAR], self.recv.at[1, s])

    def gather_left(self, s):
        _wait_for(self.blocks.at[s, pl.ds(0, 3)], self.send.at[0, s])

    def start_added(self, s, wait):
        _wait_for(self.blocks.at[s, FAR], self.recv.at[2, s])
        for d, slot in ((0, RIGHT), (1, LEFT)):
            half = (self.top, self.low)[d]
            self.blocks[s, slot, half, :] = (wait[d] + self.halves[d, s].astype(jnp.float32)).astype(jnp.bfloat16)
            self.added(d, s).start()

    def give(self, credit, s):
        self.scatter_left(s)
        for d in (0, 1):
            pl.semaphore_signal(credit.at[d], inc=1, device_id={"tp": self.to[d]}, device_id_type=pl.DeviceIdType.MESH)

    def take(self, credit):
        for d in (0, 1):
            pl.semaphore_wait(credit.at[d], 1)

    def freed(self, s):
        _wait_for(self.blocks.at[s, FAR], self.recv.at[0, s])

    def sum_here(self, d, s):
        _wait_for(self.halves.at[0, s], self.recv.at[(3, 1)[d], s])

    def summed(self, s):
        self.freed(s)
        for d in (0, 1):
            self.sum_here(d, s)

    def scatter_left(self, s):
        _wait_for(self.blocks.at[s, pl.ds(0, 3)], self.send.at[1, s])


def _steps(n, by, body, before=None, after=None):
    def step(ts):
        for f in (before, body, after):
            for t in ts:
                if f is not None:
                    f(t)

    pl.loop(0, n // by)(lambda i: step([i * by + u for u in range(by)]))
    if n % by:
        step(range(n - n % by, n))


def _normed(wide, gain_ref):
    scale = lax.rsqrt(jnp.mean(wide * wide, -1, keepdims=True) + 1e-6)
    return (wide * scale * gain_ref[...].reshape(1, -1).astype(jnp.float32)).astype(jnp.bfloat16)


def _turned(t, cos, sin):
    wide = t.astype(jnp.float32)
    return (wide * cos + pltpu.roll(wide, HEAD // 2, 1) * sin).astype(jnp.bfloat16)


def _layer(x_ref, gain_a_ref, turn_ref, wq_ref, wk_ref, wv_ref, wo_ref, gain_m_ref, gate_ref, up_ref, down_ref, y_ref, blocks, halves, sums, wait, mine,
           send, recv, weight_sem, down_sem, credit,
           gain_a, gain_m, turn):
    rows, width = blocks.shape[2], blocks.shape[3]
    shard, half = PARTS * rows, rows // 2
    ring = Ring(blocks, halves, sums, send, recv)
    bf16, f32 = jnp.bfloat16, jnp.float32
    kv = wk_ref.shape[1] // HEAD
    group = wq_ref.shape[1] // HEAD // kv
    tokens = 4 * shard
    q_tiles = wq_ref.shape[1] // WIDE
    units = gate_ref.shape[1]

    def span(i, size):
        return pl.ds(pl.multiple_of(i * size, size), size)

    def small(i):
        return pltpu.make_async_copy((gain_a_ref, gain_m_ref, turn_ref)[i], (gain_a, gain_m, turn)[i], weight_sem.at[i])

    def load(s):
        return pltpu.make_async_copy(x_ref.at[span(s, rows), :], blocks.at[s, OWN], down_sem.at[s])

    def attention(weights, wo, queries, keys, values, cos_s, sin_s, seen, term, mix_s, top_s):
        cols = group * rows
        e = HEAD**-0.5 * LOG2E

        def weight(n):
            source = wq_ref.at[:, pl.ds(n * WIDE, WIDE)] if n < q_tiles else (wk_ref, wv_ref)[n - q_tiles]
            return pltpu.make_async_copy(source, weights.at[n], weight_sem.at[0])

        def weight_out():
            return pltpu.make_async_copy(wo_ref, wo, weight_sem.at[1])

        ring.greet()
        for s in range(PARTS):
            load(s).start()
        for i in range(3):
            small(i).start()
        for i in range(3):
            small(i).wait()
        for s in range(PARTS):
            load(s).wait()
            wide = blocks[s, OWN].astype(f32)
            mine[s] = wide
            blocks[s, OWN] = _normed(wide, gain_a)
            if s == 0:
                ring.met()
            if s < 2:
                ring.start_own(s)
            if s == 1:
                for n in range(q_tiles + 2):
                    weight(n).start()
                weight_out().start()

        @pl.loop(0, tokens // shard)
        def _(i):
            at = span(i, shard)
            angle = (lax.broadcasted_iota(jnp.int32, (shard, HEAD), 0) + i * shard).astype(f32) * turn[...]
            cos_s[at, :] = jnp.cos(angle)
            sine = jnp.sin(angle)
            sin_s[at, :] = jnp.where(lax.broadcasted_iota(jnp.int32, (shard, HEAD), 1) < HEAD // 2, -sine, sine)

        keys[...] = jnp.zeros(keys.shape, bf16)
        values[:, :HEAD, :] = jnp.zeros((kv, HEAD, tokens), bf16)
        values[:, HEAD:, :] = jnp.ones((kv, values.shape[1] - HEAD, tokens), bf16)
        _wait_for(weights, weight_sem.at[0])

        def project(s, first, count):
            places = [pl.ds(pl.multiple_of(lax.rem(ring.me + k + 3, 4) * shard + s * rows, rows), rows) for k in range(first, first + count)]

            def tile(n):
                rows_of = blocks[s, first : first + count].reshape(count * rows, width)
                return jnp.dot(rows_of, weights[n], preferred_element_type=f32).astype(bf16)

            def piece(t, k, i):
                return t[k * rows : (k + 1) * rows, i * HEAD : (i + 1) * HEAD]

            @pl.loop(0, q_tiles)
            def _(n):
                t = tile(n)
                for k in range(count):
                    for i in range(WIDE // HEAD):
                        head = n * (WIDE // HEAD) + i
                        turned = _turned(piece(t, k, i), cos_s[places[k], :], sin_s[places[k], :])
                        queries[lax.div(head, group), s, first + k, lax.rem(head, group)] = turned

            t = tile(q_tiles)
            for k in range(count):
                for i in range(kv):
                    keys[i, places[k], :] = _turned(piece(t, k, i), cos_s[places[k], :], sin_s[places[k], :])
            t = tile(q_tiles + 1)
            for k in range(count):
                for i in range(kv):
                    values[i, :HEAD, places[k]] = piece(t, k, i).T

        @pl.loop(0, PARTS)
        def _(s):
            ring.pass_on(s)

            @pl.when(s < PARTS - 2)
            def _():
                ring.start_own(s + 2)

            project(s, LEFT, 3)

            @pl.when((s >= 1) & (s < PARTS - 1))
            def _():
                ring.gathered(s - 1)
                project(s - 1, FAR, 1)

        weight_out().wait()

        def attend_part(k, s):
            last = lax.rem(ring.me + k + 3, 4)
            for i in range(kv):
                top_s[i : i + 1, :] = jnp.full((1, cols), NEG, f32)
                mix_s[i] = jnp.zeros(mix_s.shape[1:], f32)

            def block(j, masked):
                here = span(j, shard)
                scores = [_dot(keys[i, here, :], queries[i, s, k].reshape(cols, HEAD), 1, 1) for i in range(kv)]
                if masked:
                    place = lax.rem(lax.broadcasted_iota(jnp.int32, (shard, cols), 1), rows) + s * rows
                    ok = lax.broadcasted_iota(jnp.int32, (shard, cols), 0) <= place
                soft, keeps = [], []
                for i in range(kv):
                    w = jnp.where(ok, scores[i], HIDDEN) if masked else scores[i]
                    old = top_s[i : i + 1, :]
                    top = jnp.maximum(old, w.max(axis=0, keepdims=True))
                    top_s[i : i + 1, :] = top
                    soft.append(jnp.exp2((w - top) * e).astype(bf16))
                    keeps.append(jnp.exp2((old - top) * e))
                for i in range(kv):
                    mix_s[i] = mix_s[i] * keeps[i] + _dot(values[i, :, here], soft[i], 1, 0)

            lax.fori_loop(0, last, lambda j, _: block(j, False), None)
            block(last, True)
            for i in range(kv):
                out = (mix_s[i, :HEAD, :] * (1 / mix_s[i, HEAD : HEAD + 1, :])).T.astype(bf16)
                for n in range(group):
                    at = (i * group + n) * HEAD
                    seen[:, at : at + HEAD] = out[n * rows : (n + 1) * rows]

            @pl.loop(0, 2)
            def _(n):
                at = span(n, width // 2)
                term[:, at] = jnp.dot(seen[...], wo[:, at], preferred_element_type=f32)

        @pl.loop(0, 2 + 3 * PARTS)
        def _(j):
            m, r = lax.div(j - 2, 3), lax.rem(j - 2, 3)
            early = j < 2
            kind = jnp.where(early, 0, r)
            s = jnp.where(early, j, jnp.where(r == 0, m + 2, m))

            @pl.when(s < PARTS)
            def _():
                attend_part(jnp.where(kind == 0, FAR, jnp.where(kind == 1, RIGHT, LEFT)), s)

                @pl.when(kind == 0)
                def _():
                    blocks[s, FAR] = term[...].astype(bf16)
                    for d in (0, 1):
                        ring.far(d, s).start()

                @pl.when(kind == 1)
                def _():
                    wait[0, 0] = term[:half, :]
                    blocks[s, RIGHT, half:, :] = term[half:, :].astype(bf16)
                    ring.free(0, s).start()

                @pl.when(kind == 2)
                def _():
                    wait[0, 1] = term[half:, :]
                    blocks[s, LEFT, :half, :] = term[:half, :].astype(bf16)
                    ring.free(1, s).start()

                    @pl.when(s < PARTS - 1)
                    def _():
                        ring.start_added(s, wait.at[0])

            @pl.when(early)
            def _():
                ring.gathered(j + 2)
                project(j + 2, FAR, 1)

            @pl.when(j == 1)
            def _():
                for p in range(PARTS):
                    ring.gather_left(p)

        @pl.loop(0, PARTS)
        def _(s):
            attend_part(OWN, s)
            mine[s] = mine[s] + term[...]

            @pl.when(s == 0)
            def _():
                ring.start_added(PARTS - 1, wait.at[0])

    pl.run_scoped(
        attention,
        pltpu.VMEM((q_tiles + 2, width, WIDE), bf16),
        pltpu.VMEM(wo_ref.shape, bf16),
        pltpu.VMEM((kv, PARTS, 4, group, rows, HEAD), bf16),
        pltpu.VMEM((kv, tokens, HEAD), bf16),
        pltpu.VMEM((kv, HEAD + 16, tokens), bf16),
        pltpu.VMEM((tokens, HEAD), f32),
        pltpu.VMEM((tokens, HEAD), f32),
        pltpu.VMEM((rows, wo_ref.shape[0]), bf16),
        pltpu.VMEM((rows, width), f32),
        pltpu.VMEM((kv, HEAD + 16, group * rows), f32),
        pltpu.VMEM((kv, group * rows), f32),
    )

    def mlp(hidden, both, down):
        tiles, steps = both.shape[0], width // WIDE

        def weight(t, i):
            return pltpu.make_async_copy((gate_ref, up_ref)[i].at[:, span(t, 128)], both.at[t, :, pl.ds(i * 128, 128)], weight_sem.at[0])

        def down_tile(g):
            slot = lax.rem(g, SLOTS)
            return pltpu.make_async_copy(down_ref.at[:, span(lax.rem(g, steps), WIDE)], down.at[slot], down_sem.at[slot])

        @pl.loop(0, tiles)
        def _(t):
            weight(t, 0).start()
            weight(t, 1).start()

        for g in range(SLOTS):
            down_tile(g).start()

        def finish(s):
            ring.summed(s)
            ring.give(credit, s)
            h = (mine[s] + sums[0, s].astype(f32) + sums[1, s].astype(f32)).astype(bf16).astype(f32)
            mine[s] = h
            blocks[s, OWN] = _normed(h, gain_m)

        for s in range(PARTS):
            finish(s)
            if s < 2:
                ring.take(credit)
                ring.start_own(s)
        for s in range(2, PARTS):
            ring.pass_on(s - 2)
            ring.take(credit)
            ring.start_own(s)

        for s in range(PARTS):
            ring.gathered(s)

            def gate_up(t):
                gu = jnp.dot(blocks[s].reshape(4 * rows, width), both[t], preferred_element_type=f32)
                gate, up = gu[:, :128], gu[:, 128:]
                hidden[:, span(t, 128)] = (gate * jax.nn.sigmoid(gate) * up).astype(bf16)

            if s == 0:
                _wait_for(both, weight_sem.at[0])
            _steps(tiles, GATE_STEP, gate_up)
            if s == 1:
                ring.pass_on(3)
            ring.gather_left(s)

            def bring_down(n):
                g = s * steps + n
                at = span(n, WIDE)
                out = jnp.dot(hidden[...], down[lax.rem(g, SLOTS)], preferred_element_type=f32)
                left, own, right, far = (out[k * rows : (k + 1) * rows] for k in range(4))
                blocks[s, FAR, :, at] = far.astype(bf16)
                wait[s % 2, 0, :, at] = right[:half]
                blocks[s, RIGHT, half:, at] = right[half:].astype(bf16)
                blocks[s, LEFT, :half, at] = left[:half].astype(bf16)
                wait[s % 2, 1, :, at] = left[half:]
                mine[s, :, at] = mine[s, :, at] + own

            def down_next(n):
                g = s * steps + n

                @pl.when(g + SLOTS < PARTS * steps)
                def _():
                    down_tile(g + SLOTS).start()

            _steps(steps, DOWN_STEP, bring_down, lambda n: down_tile(s * steps + n).wait(), down_next)
            if s == 0:
                ring.pass_on(2)
            for d in (0, 1):
                ring.far(d, s).start()
            for d in (0, 1):
                ring.free(d, s).start()
            if s >= 1:
                ring.start_added(s - 1, wait.at[(s - 1) % 2])

        for s in range(PARTS):
            if s == 1:
                ring.start_added(PARTS - 1, wait.at[(PARTS - 1) % 2])
            ring.freed(s)
            mine[s, ring.top, :] = mine[s, ring.top, :] + sums[1, s, ring.top, :].astype(f32)
            mine[s, ring.low, :] = mine[s, ring.low, :] + sums[0, s, ring.low, :].astype(f32)
            for d in (0, 1):
                ring.sum_here(d, s)
                part = (ring.top, ring.low)[d]
                at = s * rows + d * half
                y_ref[at : at + half, :] = (mine[s, part, :] + sums[d, s, part, :].astype(f32)).astype(bf16)
        for s in range(PARTS):
            ring.scatter_left(s)

    pl.run_scoped(
        mlp,
        pltpu.VMEM((4 * rows, units), bf16),
        pltpu.VMEM((units // 128, width, 256), bf16),
        pltpu.VMEM((SLOTS, units, WIDE), bf16),
    )


def layer(x, gain_a, wq, wk, wv, wo, gain_m, w_gate, w_up, w_down):
    tokens, width = x.shape
    rows, units = tokens // PARTS, w_gate.shape[1]
    turn = (float(THETA) ** (-np.arange(HEAD // 2) / (HEAD // 2))).astype(np.float32)
    turn = jnp.asarray(np.concatenate([turn, turn])[None])
    anywhere, vmem = pl.BlockSpec(memory_space=pl.ANY), pl.BlockSpec(memory_space=pltpu.VMEM)
    bf16, f32 = jnp.bfloat16, jnp.float32
    return pl.pallas_call(
        _layer,
        in_specs=[anywhere] * 11,
        out_specs=vmem,
        out_shape=pltpu.VMEM(x.shape, bf16),
        scratch_shapes=[
            pltpu.VMEM((PARTS, 4, rows, width), bf16),
            pltpu.VMEM((2, PARTS, rows // 2, width), bf16),
            pltpu.VMEM((2, PARTS, rows, width), bf16),
            pltpu.VMEM((2, 2, rows // 2, width), f32),
            pltpu.VMEM((PARTS, rows, width), f32),
            pltpu.SemaphoreType.DMA((2, PARTS)),
            pltpu.SemaphoreType.DMA((4, PARTS)),
            pltpu.SemaphoreType.DMA((3,)),
            pltpu.SemaphoreType.DMA((max(SLOTS, PARTS),)),
            pltpu.SemaphoreType.REGULAR((2,)),
            pltpu.VMEM(gain_a.shape, bf16),
            pltpu.VMEM(gain_m.shape, bf16),
            pltpu.VMEM(turn.shape, f32),
        ],
        compiler_params=pltpu.CompilerParams(collective_id=0, has_side_effects=True, vmem_limit_bytes=MOST),
        name="layer",
    )(x, gain_a, turn, wq, wk, wv, wo, gain_m, w_gate, w_up, w_down)


def solution(mesh):
    tokens, columns, rows_of = P(("dp", "tp"), None), P(None, "tp"), P("tp", None)
    return jax.shard_map(
        layer,
        mesh=mesh,
        in_specs=(tokens, P(None), columns, columns, columns, rows_of, P(None), columns, columns, rows_of),
        out_specs=tokens,
        check_vma=False,
    )
```
